256 devices in a mesh: tenant: 2 (over z), row: 128 (over x, y, core).
Axes of the slice: x: 8, y: 8, z: 2, core: 2. Of those that a mesh axis runs over, the one named last changes fastest.
The devices are a block of a 8x8x16 slice.
Arguments:
- queries: bfloat16 [32768, 256], P(('tenant', 'row')), parts along dimension 0, may hold values from -6 to 6
- probes: int32 [32768, 16], P(('tenant', 'row')), parts along dimension 0, may hold values from 0 to 1039, all different within a row; in each aligned block of 128 rows (0 to 127, 128 to 255, ...) at most 4 rows name the same one
- hot_lists: bfloat16 [32, 256, 256], P('tenant'), parts along dimension 0, may hold values from -0.375 to 0.375
- cold_lists: bfloat16 [2048, 256, 256], P(('tenant', 'row')), parts along dimension 0, may hold values from -0.375 to 0.375
Outputs:
- nearest: float32 [32768, 128], P(('tenant', 'row')), parts along dimension 0
The draws below stay inside these ranges and needn't reach their ends.
There are 2 independent parts, one for each index of `tenant`. The reference program is written for one: setup_inputs(seed, part) draws one part's arguments, and reference() takes and returns one part's arrays. A program takes and returns all parts, laid end to end along the dimension named above; each array names one. Nothing has to cross between parts.
Inputs may be any that keep to these rules, and one draw needn't show every extreme that they name: `probes`: each query names 16 different lists; every list is named by some query. Within the queries of one index of row (aligned blocks of 128 rows) no list is named more than 4 times, a bound that some block reaches.
All inputs are finite; a program needn't handle non-finite values.
Results may differ from the reference program's by a relative error of at most 0.0003.
Values may be sent and summed in bfloat16 or wider, within the bound.
A program may use at most 64 MiB of HBM per device.

```python
import math
import jax
import jax.numpy as jnp
import numpy as np
from jax import lax

DIM = 256
LSIZE = 256
NPROBE = 16
TOPK = 128
HOT = 16
QDEV = 128
COLD = 1024
NLIST = 1040
QUERIES = 16384
CAP = 4
N_ROW = 128


def block_levels(stream_key, dims, cuts, low, top_value):
    loudness = 1.0
    for dim, blocks in cuts:
        draws = jax.random.uniform(jax.random.fold_in(jax.random.fold_in(stream_key, 6), dim), (blocks,), jnp.float32, low / len(cuts), top_value / len(cuts))
        loudness = loudness * jnp.repeat(jnp.exp(draws), dims[dim] // blocks).reshape((-1,) + (1,) * (len(dims) - 1 - dim))
    return loudness


def assign_block(key, own, number, rows, count, top, bound, lean):
    order = jax.random.permutation(key, count)
    heavy_load, ordinary = portions_of(count, rows * top, bound, lean, True), portions_of(count, rows * top, bound, lean, False)
    places = jnp.arange(count)

    def named(tallies, rotation):
        used = int((tallies > 0).sum())
        fixed = max(1, used // 4)
        passed = fixed + (places - fixed + rotation * (used - fixed)) % max(1, count - fixed)
        return jnp.zeros((count,), jnp.int32).at[order[jnp.where(places < fixed, places, passed)]].set(jnp.asarray(tallies, jnp.int32))

    tallies = jnp.where(number % 4 == 0, named(heavy_load, number // 4), named(ordinary, number - number // 4 - 1))
    mixed = jax.random.permutation(jax.random.fold_in(own, 3), count)
    donor, receiver = mixed[0:count // 2 * 2:2], mixed[1:count // 2 * 2:2]
    slack = jnp.minimum(tallies[donor] - 1, bound - tallies[receiver]) // 2
    slack = jnp.where((donor == order[0]) | (receiver == order[0]) | (tallies[receiver] == 0), 0, jnp.maximum(slack, 0))
    passed = jax.random.randint(jax.random.fold_in(own, 4), (count // 2,), 0, 1 << 20) % (slack + 1)
    tallies = tallies.at[donor].add(-passed).at[receiver].add(passed)
    members = jnp.searchsorted(jnp.cumsum(tallies), jnp.arange(rows * top), side="right").astype(jnp.int32)
    grid = members.reshape(top, rows).T
    grid = grid[jax.random.permutation(jax.random.fold_in(own, 1), rows)]
    rotation = jax.random.randint(jax.random.fold_in(own, 2), (rows, 1), 0, top)
    return jnp.take_along_axis(grid, (jnp.arange(top)[None, :] + rotation) % top, axis=1)


def portions_of(amount, total, bound, skew, full):
    portions = [(1 << 20) // math.isqrt(standing ** skew) + 1 for standing in range(1, amount + 1)]
    largest = bound if full else min(bound, max(-(-total // amount), total * portions[0] // sum(portions)))
    least = 1 if total - largest >= amount - 1 else 0
    counts, rest = [largest] + [least] * (amount - 1), total - largest - least * (amount - 1)
    while rest > 0:
        movable = [i for i in range(1, amount) if counts[i] < largest] or [i for i in range(1, amount) if counts[i] < bound]
        mass, remaining = sum([portions[i] for i in movable]), rest
        for i in movable:
            more = min(bound - counts[i], max(1, remaining * portions[i] // mass), rest)
            counts[i] = counts[i] + more
            rest = rest - more
    return np.array(counts)


def scatter_about(rng, shape, width, limit, pieces=(), kind=jnp.bfloat16):
    array = width * jax.random.normal(rng, shape, jnp.float32)
    if pieces:
        array = array * block_levels(rng, shape, pieces, -0.22, 0.18)
    return jnp.clip(array, -limit, limit).astype(kind)


def setup_inputs(seed: int = 0, part: int = 0) -> dict:
    key_list = jax.random.split(jax.random.key(seed), 5)
    part_keys = jax.random.split(jax.random.fold_in(key_list[4], part), 5)
    queries = scatter_about(part_keys[0], (QUERIES, DIM), 1.0, 6.0, ((0, 128),))
    probes_keys = jax.random.split(jax.random.fold_in(part_keys[1], 1), QUERIES // QDEV)
    probes_turns = jax.random.permutation(jax.random.fold_in(part_keys[1], 3), QUERIES // QDEV)
    probes = jax.vmap(lambda own, number: assign_block(jax.random.fold_in(part_keys[1], 2), own, number, QDEV, NLIST, NPROBE, CAP, 2))(probes_keys, probes_turns).reshape((QUERIES, NPROBE))
    hot_lists = scatter_about(part_keys[2], (HOT, LSIZE, DIM), DIM ** -0.5, 0.375)
    cold_lists = scatter_about(part_keys[3], (COLD, LSIZE, DIM), DIM ** -0.5, 0.375, ((0, 128),))
    return {"queries": queries, "probes": probes, "hot_lists": hot_lists, "cold_lists": cold_lists}


def reference(queries, probes, hot_lists, cold_lists):
    lists = jnp.concatenate([hot_lists, cold_lists], axis=0)
    flat = probes.reshape(-1).astype(jnp.int32)
    count = flat.shape[0]
    pair_query = (jnp.arange(count, dtype=jnp.int32) // NPROBE).astype(jnp.int32)
    source = (pair_query // QDEV).astype(jnp.int32)
    keys = source * NLIST + flat
    order = jnp.argsort(keys, stable=True).astype(jnp.int32)
    sorted_keys = keys[order]
    position = jnp.zeros((count,), jnp.int32).at[order].set(jnp.arange(count, dtype=jnp.int32))
    first = jnp.searchsorted(sorted_keys, keys, side="left").astype(jnp.int32)
    column = source * CAP + (position - first)
    span = N_ROW * CAP
    table = jnp.zeros((NLIST * span,), jnp.int32).at[flat * span + column].set(pair_query)
    table = table.reshape(NLIST, span)
    group = 16
    blocks = (NLIST + group - 1) // group
    padding = blocks * group - NLIST
    lists_pad = jnp.pad(lists, ((0, padding), (0, 0), (0, 0))).reshape(blocks, group, LSIZE, DIM)
    table_pad = jnp.pad(table, ((0, padding), (0, 0))).reshape(blocks, group, span)

    def one_block(pair):
        group_lists, group_table = pair
        gathered = queries[group_table].astype(jnp.float32)
        scores = jnp.einsum("lwd,lvd->lwv", gathered, group_lists.astype(jnp.float32),
                            precision=lax.Precision.HIGHEST)
        return lax.top_k(scores, TOPK)[0]

    best = lax.map(one_block, (lists_pad, table_pad)).reshape(blocks * group, span, TOPK)
    candidates = best[flat, column].reshape(QUERIES, NPROBE * TOPK)
    return lax.top_k(candidates, TOPK)[0]
```

```python
import functools
import math

import jax
import jax.numpy as jnp
from jax import lax
from jax.experimental import pallas as pl
from jax.experimental.pallas import tpu as pltpu
from jax.sharding import PartitionSpec as P

MESH = pl.DeviceIdType.MESH
TOPK = 128
LANES = 128
SUB = 8
NEG = float("-inf")


def odd_even(n):
    pairs = []

    def merge(lo, hi, step):
        jump = step * 2
        if jump < hi - lo:
            merge(lo, hi, jump)
            merge(lo + step, hi, jump)
            pairs.extend((i, i + step) for i in range(lo + step, hi - step, jump))
        else:
            pairs.append((lo, lo + step))

    def sort(lo, hi):
        if hi - lo >= 1:
            mid = lo + (hi - lo) // 2
            sort(lo, mid)
            sort(mid + 1, hi)
            merge(lo, hi, 1)

    sort(0, n - 1)
    return pairs


def bitonic(values, distances):
    values = list(values)
    for d in distances:
        for i in range(len(values)):
            if i & d == 0:
                a, b = values[i], values[i + d]
                values[i], values[i + d] = jnp.maximum(a, b), jnp.minimum(a, b)
    return values


def row(base, i):
    return pl.ds(pl.multiple_of((base + i) * SUB, SUB), SUB)


def sort_groups(ref, groups, n=32):
    pairs = odd_even(n)

    def body(g, _):
        v = [ref[row(g * n, i), :] for i in range(n)]
        for a, b in pairs:
            v[a], v[b] = jnp.maximum(v[a], v[b]), jnp.minimum(v[a], v[b])
        for i in range(n):
            ref[row(g * n, i), :] = v[i]
        return 0

    lax.fori_loop(0, groups, body, 0)


def merge_full_32(src, dst, count):
    def body(g, _):
        base = g * 64
        for pick, at in ((jnp.maximum, 0), (jnp.minimum, 32)):
            v = [pick(src[row(base, i), :], src[row(base + 32, 31 - i), :]) for i in range(32)]
            v = bitonic(v, (16, 8, 4, 2, 1))
            for i in range(32):
                dst[row(base + at, i), :] = v[i]
        return 0

    lax.fori_loop(0, count, body, 0)


def half_64(src, a, b, outer, inner):
    v = []
    for i in range(32):
        low = outer(src[row(a, i), :], src[row(b, 63 - i), :])
        high = outer(src[row(a, i + 32), :], src[row(b, 31 - i), :])
        v.append(inner(low, high))
    return bitonic(v, (16, 8, 4, 2, 1))


def merge_full_64(src, dst, count):
    def body(g, _):
        base = g * 128
        at = 0
        for outer in (jnp.maximum, jnp.minimum):
            for inner in (jnp.maximum, jnp.minimum):
                v = half_64(src, base, base + 64, outer, inner)
                for i in range(32):
                    dst[row(base + at, i), :] = v[i]
                at += 32
        return 0

    lax.fori_loop(0, count, body, 0)


def merge_top_128(a, a0, b, b0, dst, d0, mid, shift=0):
    def first(g, _):
        v = []
        for k in range(8):
            other = b[row(b0 + 127 - g - 16 * k, 0), :]
            if shift:
                other = pltpu.roll(other, shift, 0)
            v.append(jnp.maximum(a[row(a0 + g + 16 * k, 0), :], other))
        v = bitonic(v, (4, 2, 1))
        for k in range(8):
            mid[row(g + 16 * k, 0), :] = v[k]
        return 0

    lax.fori_loop(0, 16, first, 0, unroll=2)

    def second(g, _):
        v = bitonic([mid[row(g * 16, i), :] for i in range(16)], (8, 4, 2, 1))
        for i in range(16):
            dst[row(d0 + g * 16, i), :] = v[i]
        return 0

    lax.fori_loop(0, 8, second, 0, unroll=2)


def sort_top_128(x, y, mid):
    sort_groups(x, 8)
    merge_full_32(x, y, 4)
    merge_full_64(y, x, 2)
    merge_top_128(x, 0, x, 128, y, 0, mid)


def prepare(rows, list_dev, hot, cap, probes_ref, queries_ref, block_ref, enc_ref, table):
    qcount, nprobe = probes_ref.shape
    cold = rows * list_dev
    lane = lax.broadcasted_iota(jnp.int32, (qcount, cold), 1)
    ids = (lane % rows) * list_dev + lane // rows + hot
    probes = probes_ref[...]
    named = jnp.zeros((qcount, cold), jnp.float32)
    for j in range(nprobe):
        named = jnp.where(probes[:, j : j + 1] == ids, 1.0, named)
    below = lax.broadcasted_iota(jnp.int32, (qcount, qcount), 1) < lax.broadcasted_iota(
        jnp.int32, (qcount, qcount), 0
    )
    rank = jnp.dot(
        below.astype(jnp.float32).astype(jnp.bfloat16),
        named.astype(jnp.bfloat16),
        preferred_element_type=jnp.float32,
    )
    number = lax.broadcasted_iota(jnp.int32, (qcount, cold), 0).astype(jnp.float32) + 1.0
    for r in range(cap):
        held = jnp.where((named > 0) & (rank == float(r)), number, 0.0)
        line = jnp.sum(held, axis=0, keepdims=True)
        for l in range(list_dev):
            e = l * cap + r
            table[e : e + 1, :] = line[:, l * rows : (l + 1) * rows]
    half = list_dev * cap // 2
    block_ref[0:qcount, :] = queries_ref[...]
    block_ref[qcount : qcount + half, 0:rows] = table[0:half, :].astype(jnp.bfloat16)
    block_ref[qcount : qcount + half, rows : 2 * rows] = table[half : 2 * half, :].astype(
        jnp.bfloat16
    )
    columns = lax.broadcasted_iota(jnp.int32, (qcount, LANES), 1)
    enc = jnp.zeros((qcount, LANES), jnp.float32)
    for j in range(nprobe):
        p = probes[:, j : j + 1]
        mine = jnp.sum(jnp.where(p == ids, rank, 0.0), axis=1, keepdims=True)
        pf = p.astype(jnp.float32)
        code = jnp.where(p < hot, -1.0 - pf, (pf - hot) * cap + mine)
        enc = jnp.where(columns == j, code, enc)
    enc_ref[...] = jnp.transpose(enc)[0:nprobe, :].astype(jnp.int32)


def exchange(rows, side, list_dev, cap, block_ref, lists_ref, out_ref, got, picked, x, y, mid, back,
             send_sem, own_sem, sib_sem, back_sem, ret_sem):
    me = lax.axis_index("row")
    mx, my, c = me // (2 * side), (me // 2) % side, me % 2
    chips = side * side
    depth = block_ref.shape[0]
    half = list_dev * cap // 2
    qcount = depth - half
    slots = list_dev * cap
    pairs = list_dev // 2

    def at(dx, dy, core):
        return (((mx + dx) % side) * side + (my + dy) % side) * 2 + core

    barrier = pltpu.get_barrier_semaphore()

    def greet(k, _):
        pl.semaphore_signal(barrier, 1, device_id={"row": (me + k) % rows}, device_id_type=MESH)
        return 0

    lax.fori_loop(1, rows, greet, 0)
    pl.semaphore_wait(barrier, rows - 1)

    def along(da, db):
        return at(da * (1 - c) + db * c, da * c + db * (1 - c), c)

    def push(src, da, db, to_a, to_b):
        slot = ((da - to_a) % side) * side + (db - to_b) % side
        pltpu.make_async_remote_copy(
            src, got.at[c, slot], send_sem, own_sem.at[slot],
            device_id={"row": along(to_a % side, to_b % side)}, device_id_type=MESH,
        ).start()

    def signed(d):
        return d if d <= side // 2 else d - side

    def forward(src, da, db):
        sa, sb = signed(da), signed(db)
        far = side // 2
        if db == 0:
            if sa <= 0 and -sa + 1 <= far and da != far:
                push(src, da, db, 1, 0)
            if sa >= 0 and sa + 1 <= far - 1:
                push(src, da, db, -1, 0)
        plus, minus = (far, far - 1) if da % 2 == 0 else (far - 1, far)
        came_plus = db == 0 or sb < 0
        came_minus = db == 0 or (sb > 0 and db != far)
        if came_plus and (0 if db == 0 else -sb) + 1 <= plus:
            push(src, da, db, 0, 1)
        if came_minus and (0 if db == 0 else sb) + 1 <= minus:
            push(src, da, db, 0, -1)

    def to_sibling(src, slot):
        pltpu.make_async_remote_copy(
            src, got.at[c, slot], send_sem, sib_sem.at[slot],
            device_id={"row": at(0, 0, 1 - c)}, device_id_type=MESH,
        ).start()

    forward(block_ref, 0, 0)
    to_sibling(block_ref, 0)
    got[c, 0] = block_ref[...]
    order = [(a, b) for a in range(side) for b in range(side) if (a, b) != (0, 0)]
    order.sort(key=lambda o: (abs(signed(o[0])) + abs(signed(o[1])), abs(signed(o[1])), o))
    for da, db in order:
        slot = da * side + db
        here = got.at[c, slot]
        pltpu.make_async_remote_copy(
            here, here, send_sem, own_sem.at[slot], device_id={"row": me}, device_id_type=MESH
        ).wait_recv()
        forward(here, da, db)
        to_sibling(here, slot)

    share = chips // (LANES // SUB)
    per = chips // share
    choose = (lax.broadcasted_iota(jnp.int32, (rows, LANES), 0) == me).astype(jnp.float32).astype(jnp.bfloat16)
    number = lax.broadcasted_iota(jnp.int32, (slots, qcount), 1).astype(jnp.float32) + 1.0
    odd = (lax.broadcasted_iota(jnp.int32, (lists_ref.shape[1], 2 * LANES), 1) // cap) % 2 == 1

    def batch(b, _):
        def take(k, _):
            i = b * per + k
            for t in range(2):
                slot = i if t == 0 else (i % side) * side + i // side
                here = got.at[t, slot]

                @pl.when((c != t))
                def _():
                    pltpu.make_async_remote_copy(
                        here, here, send_sem, sib_sem.at[slot], device_id={"row": me}, device_id_type=MESH
                    ).wait_recv()

                table = jnp.concatenate(
                    [got[t, slot, qcount:depth, 0:rows], got[t, slot, qcount:depth, rows : 2 * rows]], axis=0
                )
                wide = jnp.dot(table, choose, preferred_element_type=jnp.float32)
                hits = (wide == number).astype(jnp.float32).astype(jnp.bfloat16)
                chosen = jnp.dot(hits, got[t, slot, 0:qcount, :], preferred_element_type=jnp.float32)
                for m in range(pairs):
                    picked[m, pl.ds(pl.multiple_of(t * LANES + k * SUB, SUB), SUB), :] = chosen[
                        m * SUB : (m + 1) * SUB, :
                    ]
            return 0

        lax.fori_loop(0, per, take, 0)

        for m in range(pairs):
            right = picked[m].astype(jnp.bfloat16)
            dims = (((1,), (1,)), ((), ()))
            even_s = lax.dot_general(lists_ref[2 * m], right, dims, preferred_element_type=jnp.float32)
            odd_s = lax.dot_general(lists_ref[2 * m + 1], right, dims, preferred_element_type=jnp.float32)
            s = jnp.where(odd, odd_s, even_s)
            for t in range(2):
                x[pl.ds(2 * m + t, s.shape[0], stride=SUB), :] = s[:, t * LANES : (t + 1) * LANES]
        sort_top_128(x, y, mid)
        for m in range(pairs):
            for t in range(2):
                sorted_rows = jnp.transpose(y[pl.ds(2 * m + t, TOPK, stride=SUB), :])
                back[pl.ds(b * per, per), t, m * SUB : (m + 1) * SUB, :] = sorted_rows.reshape(per, SUB, TOPK)

        def give(k, _):
            i = b * per + k
            for t in range(2):

                @pl.when((i != 0) | (c != t))
                def _():
                    pltpu.make_async_remote_copy(
                        back.at[i, t], out_ref.at[me], back_sem, ret_sem,
                        device_id={"row": at(i // side, i % side, t)}, device_id_type=MESH,
                    ).start()
            return 0

        lax.fori_loop(0, per, give, 0)
        return 0

    lax.fori_loop(0, share, batch, 0)
    out_ref[me] = back[0, c]

    def drain(k, _):
        here = got.at[c, 0]
        pltpu.make_async_remote_copy(
            here, here, send_sem, own_sem.at[0], device_id={"row": me}, device_id_type=MESH
        ).wait_send()
        return 0

    lax.fori_loop(0, 2 * chips - 1, drain, 0)
    whole = out_ref.at[pl.ds(0, rows - 1)]
    done = pltpu.make_async_remote_copy(
        whole, whole, back_sem, ret_sem, device_id={"row": me}, device_id_type=MESH
    )
    done.wait_send()
    done.wait_recv()


def finish(enc_smem, enc_ref, rows_ref, queries_ref, hot_ref, out_ref, buf, x, y, mid, lists_a, lists_b):
    nprobe, qcount = enc_ref.shape
    hot = hot_ref.shape[0]
    enc = enc_ref[...]

    def gather(j, _):
        def one(q, _):
            at = jnp.maximum(enc_smem[j, q], 0)
            buf[pl.ds(j * qcount + q, 1), :] = rows_ref[pl.ds(at, 1), :]
            return 0

        lax.fori_loop(0, qcount, one, 0, unroll=16)
        return 0

    lax.fori_loop(0, nprobe, gather, 0)
    for j in range(nprobe):
        dst = lists_a if j < SUB else lists_b
        flat = jnp.transpose(buf[j * qcount : (j + 1) * qcount, :])
        flat = jnp.where(enc[j : j + 1, :] < 0, NEG, flat)
        dst[pl.ds(j % SUB, TOPK, stride=SUB), :] = flat
    merge_top_128(lists_a, 0, lists_b, 0, lists_a, 0, mid)
    for g in range(hot // SUB):
        for s in range(SUB):
            h = g * SUB + s
            scores = lax.dot_general(
                hot_ref[h], queries_ref[...], (((1,), (1,)), ((), ())), preferred_element_type=jnp.float32
            )
            asked = jnp.max((enc == -1 - h).astype(jnp.float32), axis=0, keepdims=True)
            x[pl.ds(s, scores.shape[0], stride=SUB), :] = jnp.where(asked > 0, scores, NEG)
        sort_top_128(x, y, mid)
        merge_top_128(lists_a, 0, y, 0, lists_a, 0, mid)
    for shift in (4, 2, 1):
        merge_top_128(lists_a, 0, lists_a, 0, lists_b, 0, mid, shift)
        lists_a, lists_b = lists_b, lists_a
    out_ref[...] = jnp.transpose(lists_a[pl.ds(0, TOPK, stride=SUB), :])


def shards(queries, probes, hot_lists, cold_lists):
    rows = lax.axis_size("row")
    side = math.isqrt(rows // 2)
    qcount, nprobe = probes.shape
    width = queries.shape[1]
    list_dev, lsize = cold_lists.shape[0], cold_lists.shape[1]
    hot = hot_lists.shape[0]
    cap = 2 * ((qcount * nprobe + list_dev * rows - 1) // (list_dev * rows))
    slots = list_dev * cap
    depth = qcount + slots // 2
    vmem = pl.BlockSpec(memory_space=pltpu.VMEM)
    limit = 60 * 2**20
    f32 = jnp.float32
    column = pltpu.VMEM((lsize * SUB, LANES), f32)
    small = pltpu.VMEM((TOPK * SUB, LANES), f32)

    block, enc = pl.pallas_call(
        functools.partial(prepare, rows, list_dev, hot, cap),
        out_shape=(
            jax.ShapeDtypeStruct((depth, width), jnp.bfloat16),
            jax.ShapeDtypeStruct((nprobe, qcount), jnp.int32),
        ),
        in_specs=[vmem] * 2,
        out_specs=(vmem, vmem),
        scratch_shapes=[pltpu.VMEM((slots, rows), f32)],
        compiler_params=pltpu.CompilerParams(vmem_limit_bytes=limit),
    )(probes, queries)

    returned = pl.pallas_call(
        functools.partial(exchange, rows, side, list_dev, cap),
        out_shape=jax.ShapeDtypeStruct((rows, slots, TOPK), f32),
        in_specs=[vmem] * 2,
        out_specs=vmem,
        scratch_shapes=[
            pltpu.VMEM((2, side * side, depth, width), jnp.bfloat16),
            pltpu.VMEM((list_dev // 2, 2 * LANES, width), f32),
            column,
            column,
            small,
            pltpu.VMEM((side * side, 2, slots, TOPK), f32),
            pltpu.SemaphoreType.DMA,
            pltpu.SemaphoreType.DMA((side * side,)),
            pltpu.SemaphoreType.DMA((side * side,)),
            pltpu.SemaphoreType.DMA,
            pltpu.SemaphoreType.DMA,
        ],
        compiler_params=pltpu.CompilerParams(collective_id=0, has_side_effects=True, vmem_limit_bytes=limit),
    )(block, cold_lists)

    return pl.pallas_call(
        finish,
        out_shape=jax.ShapeDtypeStruct((qcount, TOPK), f32),
        in_specs=[pl.BlockSpec(memory_space=pltpu.SMEM)] + [vmem] * 4,
        out_specs=vmem,
        scratch_shapes=[pltpu.VMEM((nprobe * qcount, TOPK), f32), column, column, small, small, small],
        compiler_params=pltpu.CompilerParams(vmem_limit_bytes=limit),
    )(enc, enc, returned.reshape(rows * slots, TOPK), queries, hot_lists)


def solution(mesh):
    placed = (
        P(("tenant", "row"), None),
        P(("tenant", "row"), None),
        P("tenant", None, None),
        P(("tenant", "row"), None, None),
    )
    return jax.shard_map(
        shards, mesh=mesh, in_specs=placed, out_specs=P(("tenant", "row"), None), check_vma=False
    )
```

```python
import functools
import math

import jax
import jax.numpy as jnp
from jax import lax
from jax.experimental import pallas as pl
from jax.experimental.pallas import tpu as pltpu
from jax.sharding import PartitionSpec as P

MESH = pl.DeviceIdType.MESH
TOPK = 128
LANES = 128
SUB = 8
NEG = float("-inf")


def odd_even(n):
    pairs = []

    def merge(lo, hi, step):
        jump = step * 2
        if jump < hi - lo:
            merge(lo, hi, jump)
            merge(lo + step, hi, jump)
            pairs.extend((i, i + step) for i in range(lo + step, hi - step, jump))
        else:
            pairs.append((lo, lo + step))

    def sort(lo, hi):
        if hi - lo >= 1:
            mid = lo + (hi - lo) // 2
            sort(lo, mid)
            sort(mid + 1, hi)
            merge(lo, hi, 1)

    sort(0, n - 1)
    return pairs


def bitonic(values, distances):
    values = list(values)
    for d in distances:
        for i in range(len(values)):
            if i & d == 0:
                a, b = values[i], values[i + d]
                values[i], values[i + d] = jnp.maximum(a, b), jnp.minimum(a, b)
    return values


def row(base, i):
    return pl.ds(pl.multiple_of((base + i) * SUB, SUB), SUB)


def sort_groups(ref, start, stop, n=32):
    pairs = odd_even(n)

    def body(g, _):
        v = [ref[row(g * n, i), :] for i in range(n)]
        for a, b in pairs:
            v[a], v[b] = jnp.maximum(v[a], v[b]), jnp.minimum(v[a], v[b])
        for i in range(n):
            ref[row(g * n, i), :] = v[i]
        return 0

    lax.fori_loop(start, stop, body, 0)


def merge_full_32(src, dst, count):
    def body(g, _):
        base = g * 64
        for pick, at in ((jnp.maximum, 0), (jnp.minimum, 32)):
            v = [pick(src[row(base, i), :], src[row(base + 32, 31 - i), :]) for i in range(32)]
            v = bitonic(v, (16, 8, 4, 2, 1))
            for i in range(32):
                dst[row(base + at, i), :] = v[i]
        return 0

    lax.fori_loop(0, count, body, 0)


def half_64(src, a, b, outer, inner):
    v = []
    for i in range(32):
        low = outer(src[row(a, i), :], src[row(b, 63 - i), :])
        high = outer(src[row(a, i + 32), :], src[row(b, 31 - i), :])
        v.append(inner(low, high))
    return bitonic(v, (16, 8, 4, 2, 1))


def merge_full_64(src, dst, count):
    def body(g, _):
        base = g * 128
        at = 0
        for outer in (jnp.maximum, jnp.minimum):
            for inner in (jnp.maximum, jnp.minimum):
                v = half_64(src, base, base + 64, outer, inner)
                for i in range(32):
                    dst[row(base + at, i), :] = v[i]
                at += 32
        return 0

    lax.fori_loop(0, count, body, 0)


def merge_top_128(a, a0, b, b0, dst, d0, mid, shift=0):
    def first(g, _):
        v = []
        for k in range(8):
            other = b[row(b0 + 127 - g - 16 * k, 0), :]
            if shift:
                other = pltpu.roll(other, shift, 0)
            v.append(jnp.maximum(a[row(a0 + g + 16 * k, 0), :], other))
        v = bitonic(v, (4, 2, 1))
        for k in range(8):
            mid[row(g + 16 * k, 0), :] = v[k]
        return 0

    lax.fori_loop(0, 16, first, 0, unroll=2)

    def second(g, _):
        v = bitonic([mid[row(g * 16, i), :] for i in range(16)], (8, 4, 2, 1))
        for i in range(16):
            dst[row(d0 + g * 16, i), :] = v[i]
        return 0

    lax.fori_loop(0, 8, second, 0, unroll=2)


def sort_top_128(x, y, mid):
    sort_groups(x, 0, 4)
    yield
    sort_groups(x, 4, 8)
    yield
    merge_full_32(x, y, 4)
    yield
    merge_full_64(y, x, 2)
    yield
    merge_top_128(x, 0, x, 128, y, 0, mid)
    yield


def exchange(rows, side, cap, probes_ref, queries_ref, lists_ref, hot_ref, out_ref, enc_ref, hot_out, block, table, ranks,
             got, picked, x, y, mid, back, send_sem, own_sem, sib_sem, back_sem, ret_sem):
    me = lax.axis_index("row")
    mx, my, c = me // (2 * side), (me // 2) % side, me % 2
    chips = side * side
    list_dev, lsize = lists_ref.shape[0], lists_ref.shape[1]
    hot = hot_ref.shape[0]
    nprobe, qcount = probes_ref.shape
    slots = list_dev * cap
    half = slots // 2
    depth = qcount + half
    pairs = list_dev // 2
    cold = rows * list_dev
    f32, bf16 = jnp.float32, jnp.bfloat16
    last = (((1,), (1,)), ((), ()))

    def at(dx, dy, core):
        return (((mx + dx) % side) * side + (my + dy) % side) * 2 + core

    barrier = pltpu.get_barrier_semaphore()

    def greet(k, _):
        pl.semaphore_signal(barrier, 1, device_id={"row": (me + k) % rows}, device_id_type=MESH)
        return 0

    lax.fori_loop(1, rows, greet, 0)

    wide_probes = jnp.concatenate(
        [probes_ref[...].astype(f32), jnp.zeros((LANES - nprobe, qcount), f32)], axis=0
    )
    probes = jnp.transpose(wide_probes)
    lane = lax.broadcasted_iota(jnp.int32, (qcount, cold), 1)
    ids = ((lane % rows) * list_dev + lane // rows + hot).astype(f32)
    named = jnp.zeros((qcount, cold), f32)
    for j in range(nprobe):
        named = jnp.where(probes[:, j : j + 1] == ids, 1.0, named)
    below = lax.broadcasted_iota(jnp.int32, (qcount, qcount), 1) < lax.broadcasted_iota(
        jnp.int32, (qcount, qcount), 0
    )
    rank = jnp.dot(below.astype(f32).astype(bf16), named.astype(bf16), preferred_element_type=f32)
    ranks[...] = rank
    order_of = lax.broadcasted_iota(jnp.int32, (qcount, cold), 0).astype(f32) + 1.0
    for r in range(cap):
        held = jnp.where((named > 0) & (rank == float(r)), order_of, 0.0)
        line = jnp.sum(held, axis=0, keepdims=True)
        for l in range(list_dev):
            e = l * cap + r
            table[e : e + 1, :] = line[:, l * rows : (l + 1) * rows]
    block[qcount:depth, 0:rows] = table[0:half, :].astype(bf16)
    block[qcount:depth, rows : 2 * rows] = table[half : 2 * half, :].astype(bf16)
    block[0:qcount, :] = queries_ref[...]
    got[c, 0] = block[...]

    pl.semaphore_wait(barrier, rows - 1)

    def along(da, db):
        return at(da * (1 - c) + db * c, da * c + db * (1 - c), c)

    def push(src, da, db, to_a, to_b):
        slot = ((da - to_a) % side) * side + (db - to_b) % side
        pltpu.make_async_remote_copy(
            src, got.at[c, slot], send_sem, own_sem.at[slot],
            device_id={"row": along(to_a % side, to_b % side)}, device_id_type=MESH,
        ).start()

    def signed(d):
        return d if d <= side // 2 else d - side

    def forward(src, da, db):
        sa, sb = signed(da), signed(db)
        far = side // 2
        if db == 0:
            if sa <= 0 and -sa + 1 <= far:
                push(src, da, db, 1, 0)
            if sa >= 0 and sa + 1 <= far - 1:
                push(src, da, db, -1, 0)
        plus, minus = (far, far - 1) if da % 2 == 0 else (far - 1, far)
        came_plus = db == 0 or sb < 0
        came_minus = db == 0 or (sb > 0 and db != far)
        if came_plus and (0 if db == 0 else -sb) + 1 <= plus:
            push(src, da, db, 0, 1)
        if came_minus and (0 if db == 0 else sb) + 1 <= minus:
            push(src, da, db, 0, -1)

    def to_sibling(src, slot):
        pltpu.make_async_remote_copy(
            src, got.at[c, slot], send_sem, sib_sem.at[slot],
            device_id={"row": at(0, 0, 1 - c)}, device_id_type=MESH,
        ).start()

    def await_block(t, slot, sem):
        here = got.at[t, slot]
        pltpu.make_async_remote_copy(
            here, here, send_sem, sem.at[slot], device_id={"row": me}, device_id_type=MESH
        ).wait_recv()

    order = [(a, b) for a in range(side) for b in range(side)]
    order.sort(key=lambda o: (abs(signed(o[0])) + abs(signed(o[1])), abs(signed(o[1])), o))
    per = LANES // SUB
    step = 4

    choose = (lax.broadcasted_iota(jnp.int32, (rows, LANES), 0) == me).astype(f32).astype(bf16)
    number = lax.broadcasted_iota(jnp.int32, (slots, qcount), 1).astype(f32) + 1.0
    odd = (lax.broadcasted_iota(jnp.int32, (lsize, 2 * LANES), 1) // cap) % 2 == 1

    def slot_of(t, chip):
        return chip[t] * side + chip[1 - t]

    def positions():
        columns = lax.broadcasted_iota(jnp.int32, (qcount, LANES), 1)
        enc = jnp.zeros((qcount, LANES), f32)
        for j in range(nprobe):
            p = probes[:, j : j + 1]
            mine = jnp.sum(jnp.where(p == ids, ranks[...], 0.0), axis=1, keepdims=True)
            code = jnp.where(p < hot, -1.0 - p, (p - hot) * cap + mine)
            enc = jnp.where(columns == j, code, enc)
        enc_ref[...] = jnp.transpose(enc)[0:nprobe, :].astype(jnp.int32)
        yield

    def hot_work():
        for g in range(hot // SUB):
            for s in range(SUB):
                h = g * SUB + s
                scores = lax.dot_general(hot_ref[h], queries_ref[...], last, preferred_element_type=f32)
                asked = jnp.max((probes_ref[...] == h).astype(f32), axis=0, keepdims=True)
                x[pl.ds(s, lsize, stride=SUB), :] = jnp.where(asked > 0, scores, NEG)
                if s % 4 == 3:
                    yield
            yield from sort_top_128(x, y, mid)
            if g == 0:
                hot_out[...] = y[0 : TOPK * SUB, :]
            else:
                merge_top_128(hot_out, 0, y, 0, hot_out, 0, mid)
            yield

    def batch(b):
        mine = order[b * per : (b + 1) * per]
        for k0 in range(0, per, step):
            some = [(k, t) for k in range(k0, k0 + step) for t in range(2)]
            for t in range(2):

                @pl.when(c != t)
                def _():
                    for k in range(k0, k0 + step):
                        await_block(t, slot_of(t, mine[k]), sib_sem)

            tables = []
            for k, t in some:
                slot = slot_of(t, mine[k])
                tables += [got[t, slot, qcount:depth, 0:rows], got[t, slot, qcount:depth, rows : 2 * rows]]
            wide = jnp.dot(jnp.concatenate(tables, axis=0), choose, preferred_element_type=f32)
            for n, (k, t) in enumerate(some):
                hits = (wide[n * slots : (n + 1) * slots, :] == number).astype(f32).astype(bf16)
                chosen = jnp.dot(hits, got[t, slot_of(t, mine[k]), 0:qcount, :], preferred_element_type=f32)
                for m in range(pairs):
                    low = t * LANES + k * SUB
                    picked[m, low : low + SUB, :] = chosen[m * SUB : (m + 1) * SUB, :]
            yield
        for m in range(pairs):
            right = picked[m].astype(bf16)
            even_s = lax.dot_general(lists_ref[2 * m], right, last, preferred_element_type=f32)
            odd_s = lax.dot_general(lists_ref[2 * m + 1], right, last, preferred_element_type=f32)
            s = jnp.where(odd, odd_s, even_s)
            for t in range(2):
                x[pl.ds(2 * m + t, lsize, stride=SUB), :] = s[:, t * LANES : (t + 1) * LANES]
            yield
        yield from sort_top_128(x, y, mid)
        for m in range(pairs):
            for t in range(2):
                sorted_rows = jnp.transpose(y[pl.ds(2 * m + t, TOPK, stride=SUB), :])
                back[b * per : (b + 1) * per, t, m * SUB : (m + 1) * SUB, :] = sorted_rows.reshape(per, SUB, TOPK)
        yield
        for k in range(per):
            dx, dy = mine[k]
            for t in range(2):

                def give():
                    pltpu.make_async_remote_copy(
                        back.at[b * per + k, t], out_ref.at[me], back_sem, ret_sem,
                        device_id={"row": at(dx, dy, t)}, device_id_type=MESH,
                    ).start()

                if (dx, dy) == (0, 0):
                    pl.when(c != t)(give)
                else:
                    give()
            if k % step == step - 1:
                yield

    forward(block, 0, 0)
    to_sibling(block, 0)

    todo = [positions(), hot_work()]
    batches = [(set(order[b * per : (b + 1) * per]), batch(b)) for b in range(chips // per)]
    passed = {(0, 0)}

    def advance(count):
        while count and (todo or batches):
            if not todo:
                need, work = batches[0]
                if not all((a, b) in passed and (b, a) in passed for a, b in need):
                    return
                batches.pop(0)
                todo.append(work)
            try:
                next(todo[0])
                count -= 1
            except StopIteration:
                todo.pop(0)

    for da, db in order[1:]:
        slot = da * side + db
        await_block(c, slot, own_sem)
        forward(got.at[c, slot], da, db)
        to_sibling(got.at[c, slot], slot)
        passed.add((da, db))
        advance(1)
    advance(1 << 20)
    out_ref[me] = back[0, c]

    def drain(k, _):
        here = got.at[c, 0]
        pltpu.make_async_remote_copy(
            here, here, send_sem, own_sem.at[0], device_id={"row": me}, device_id_type=MESH
        ).wait_send()
        return 0

    lax.fori_loop(0, 2 * chips - 1, drain, 0)
    whole = out_ref.at[pl.ds(0, rows - 1)]
    done = pltpu.make_async_remote_copy(
        whole, whole, back_sem, ret_sem, device_id={"row": me}, device_id_type=MESH
    )
    done.wait_send()
    done.wait_recv()


def finish(enc_smem, enc_ref, rows_ref, hot_ref, out_ref, buf, mid, lists_a, lists_b):
    nprobe, qcount = enc_ref.shape
    enc = enc_ref[...]

    def gather(j, _):
        def one(q, _):
            at = jnp.maximum(enc_smem[j, q], 0)
            buf[pl.ds(j * qcount + q, 1), :] = rows_ref[pl.ds(at, 1), :]
            return 0

        lax.fori_loop(0, qcount, one, 0, unroll=16)
        return 0

    lax.fori_loop(0, nprobe, gather, 0)
    for j in range(nprobe):
        dst = lists_a if j < SUB else lists_b
        flat = jnp.transpose(buf[j * qcount : (j + 1) * qcount, :])
        flat = jnp.where(enc[j : j + 1, :] < 0, NEG, flat)
        dst[pl.ds(j % SUB, TOPK, stride=SUB), :] = flat
    merge_top_128(lists_a, 0, lists_b, 0, lists_a, 0, mid)
    merge_top_128(lists_a, 0, hot_ref, 0, lists_a, 0, mid)
    for shift in (4, 2, 1):
        merge_top_128(lists_a, 0, lists_a, 0, lists_b, 0, mid, shift)
        lists_a, lists_b = lists_b, lists_a
    out_ref[...] = jnp.transpose(lists_a[pl.ds(0, TOPK, stride=SUB), :])


def shards(queries, probes, hot_lists, cold_lists):
    rows = lax.axis_size("row")
    side = math.isqrt(rows // 2)
    qcount, nprobe = probes.shape
    width = queries.shape[1]
    list_dev, lsize = cold_lists.shape[0], cold_lists.shape[1]
    hot = hot_lists.shape[0]
    cap = 2 * ((qcount * nprobe + list_dev * rows - 1) // (list_dev * rows))
    slots = list_dev * cap
    depth = qcount + slots // 2
    vmem = pl.BlockSpec(memory_space=pltpu.VMEM)
    limit = 60 * 2**20
    f32 = jnp.float32
    column = pltpu.VMEM((lsize * SUB, LANES), f32)
    small = pltpu.VMEM((TOPK * SUB, LANES), f32)

    returned, enc, hot_best = pl.pallas_call(
        functools.partial(exchange, rows, side, cap),
        out_shape=(
            jax.ShapeDtypeStruct((rows, slots, TOPK), f32),
            jax.ShapeDtypeStruct((nprobe, qcount), jnp.int32),
            jax.ShapeDtypeStruct((TOPK * SUB, LANES), f32),
        ),
        in_specs=[vmem] * 4,
        out_specs=(vmem,) * 3,
        scratch_shapes=[
            pltpu.VMEM((depth, width), jnp.bfloat16),
            pltpu.VMEM((slots, rows), f32),
            pltpu.VMEM((qcount, rows * list_dev), f32),
            pltpu.VMEM((2, side * side, depth, width), jnp.bfloat16),
            pltpu.VMEM((list_dev // 2, 2 * LANES, width), f32),
            column,
            column,
            small,
            pltpu.VMEM((side * side, 2, slots, TOPK), f32),
            pltpu.SemaphoreType.DMA,
            pltpu.SemaphoreType.DMA((side * side,)),
            pltpu.SemaphoreType.DMA((side * side,)),
            pltpu.SemaphoreType.DMA,
            pltpu.SemaphoreType.DMA,
        ],
        compiler_params=pltpu.CompilerParams(collective_id=0, has_side_effects=True, vmem_limit_bytes=limit),
    )(probes.T, queries, cold_lists, hot_lists)

    return pl.pallas_call(
        finish,
        out_shape=jax.ShapeDtypeStruct((qcount, TOPK), f32),
        in_specs=[pl.BlockSpec(memory_space=pltpu.SMEM)] + [vmem] * 3,
        out_specs=vmem,
        scratch_shapes=[pltpu.VMEM((nprobe * qcount, TOPK), f32), small, small, small],
        compiler_params=pltpu.CompilerParams(vmem_limit_bytes=limit),
    )(enc, enc, returned.reshape(rows * slots, TOPK), hot_best)


def solution(mesh):
    placed = (
        P(("tenant", "row"), None),
        P(("tenant", "row"), None),
        P("tenant", None, None),
        P(("tenant", "row"), None, None),
    )
    return jax.shard_map(
        shards, mesh=mesh, in_specs=placed, out_specs=P(("tenant", "row"), None), check_vma=False
    )
```

```python
import functools
import math

import jax
import jax.numpy as jnp
from jax import lax
from jax.experimental import pallas as pl
from jax.experimental.pallas import tpu as pltpu
from jax.sharding import PartitionSpec as P

MESH = pl.DeviceIdType.MESH
TOPK = 128
FIRST = 64
LANES = 128
SUB = 8
NEG = float("-inf")


def odd_even(n):
    pairs = []

    def merge(lo, hi, step):
        jump = step * 2
        if jump < hi - lo:
            merge(lo, hi, jump)
            merge(lo + step, hi, jump)
            pairs.extend((i, i + step) for i in range(lo + step, hi - step, jump))
        else:
            pairs.append((lo, lo + step))

    def sort(lo, hi):
        if hi - lo >= 1:
            mid = lo + (hi - lo) // 2
            sort(lo, mid)
            sort(mid + 1, hi)
            merge(lo, hi, 1)

    sort(0, n - 1)
    return pairs


def bitonic(values, distances):
    values = list(values)
    for d in distances:
        for i in range(len(values)):
            if i & d == 0:
                a, b = values[i], values[i + d]
                values[i], values[i + d] = jnp.maximum(a, b), jnp.minimum(a, b)
    return values


def row(base, i):
    at = (base + i) * SUB
    return pl.ds(at if isinstance(at, int) else pl.multiple_of(at, SUB), SUB)


def sort_groups(ref, start, stop, n=32):
    pairs = odd_even(n)

    def body(g, _):
        v = [ref[row(g * n, i), :] for i in range(n)]
        for a, b in pairs:
            v[a], v[b] = jnp.maximum(v[a], v[b]), jnp.minimum(v[a], v[b])
        for i in range(n):
            ref[row(g * n, i), :] = v[i]
        return 0

    lax.fori_loop(start, stop, body, 0)


def merge_full_32(src, dst, count):
    def body(g, _):
        base = g * 64
        for pick, at in ((jnp.maximum, 0), (jnp.minimum, 32)):
            v = [pick(src[row(base, i), :], src[row(base + 32, 31 - i), :]) for i in range(32)]
            v = bitonic(v, (16, 8, 4, 2, 1))
            for i in range(32):
                dst[row(base + at, i), :] = v[i]
        return 0

    lax.fori_loop(0, count, body, 0)


def half_64(src, a, b, outer, inner):
    v = []
    for i in range(32):
        low = outer(src[row(a, i), :], src[row(b, 63 - i), :])
        high = outer(src[row(a, i + 32), :], src[row(b, 31 - i), :])
        v.append(inner(low, high))
    return bitonic(v, (16, 8, 4, 2, 1))


def merge_full_64(src, dst, count):
    def body(g, _):
        base = g * 128
        at = 0
        for outer in (jnp.maximum, jnp.minimum):
            for inner in (jnp.maximum, jnp.minimum):
                v = half_64(src, base, base + 64, outer, inner)
                for i in range(32):
                    dst[row(base + at, i), :] = v[i]
                at += 32
        return 0

    lax.fori_loop(0, count, body, 0)


def merge_top_128(a, a0, b, b0, dst, d0, mid, shift=0):
    def first(g, _):
        v = []
        for k in range(8):
            other = b[row(b0 + 127 - g - 16 * k, 0), :]
            if shift:
                other = pltpu.roll(other, shift, 0)
            v.append(jnp.maximum(a[row(a0 + g + 16 * k, 0), :], other))
        v = bitonic(v, (4, 2, 1))
        for k in range(8):
            mid[row(g + 16 * k, 0), :] = v[k]
        return 0

    lax.fori_loop(0, 16, first, 0, unroll=2)

    def second(g, _):
        v = bitonic([mid[row(g * 16, i), :] for i in range(16)], (8, 4, 2, 1))
        for i in range(16):
            dst[row(d0 + g * 16, i), :] = v[i]
        return 0

    lax.fori_loop(0, 8, second, 0, unroll=2)


def sort_top_128(x, y, mid):
    sort_groups(x, 0, 4)
    yield
    sort_groups(x, 4, 8)
    yield
    merge_full_32(x, y, 4)
    yield
    merge_full_64(y, x, 2)
    yield
    merge_top_128(x, 0, x, 128, y, 0, mid)
    yield


def sort_top_64(x, y):
    sort_groups(x, 0, 4)
    yield
    sort_groups(x, 4, 8)
    yield
    merge_full_32(x, y, 4)
    yield
    for src, dst, count in ((y, x, 2), (x, y, 1)):
        for g in range(count):
            for n, inner in enumerate((jnp.maximum, jnp.minimum)):
                v = half_64(src, g * 128, g * 128 + 64, jnp.maximum, inner)
                for i in range(32):
                    dst[row(g * 64 + n * 32, i), :] = v[i]
        yield


def run(pieces):
    for _ in pieces:
        pass


def exchange(rows, side, cap, probes_ref, queries_ref, lists_ref, hot_ref, best_ref, flag_ref, block, table, ranks,
             got, picked, x, y, mid, back, out_ref, enc_ref, line_ref, enc_smem, hot_out, buf, lists_a, lists_b, note, notes_x, notes_y,
             send_sem, own_sem, sib_sem, back_sem, ret_sem, enc_sem, note_sem, nx_sem, ny_sem):
    me = lax.axis_index("row")
    mx, my, c = me // (2 * side), (me // 2) % side, me % 2
    chips = side * side
    list_dev, lsize = lists_ref.shape[0], lists_ref.shape[1]
    hot = hot_ref.shape[0]
    nprobe, qcount = probes_ref.shape
    slots = list_dev * cap
    half = slots // 2
    depth = qcount + half
    pairs = list_dev // 2
    cold = rows * list_dev
    f32, bf16 = jnp.float32, jnp.bfloat16
    last = (((1,), (1,)), ((), ()))

    def at(dx, dy, core):
        return (((mx + dx) % side) * side + (my + dy) % side) * 2 + core

    barrier = pltpu.get_barrier_semaphore()

    def greet(k, _):
        pl.semaphore_signal(barrier, 1, device_id={"row": (me + k) % rows}, device_id_type=MESH)
        return 0

    lax.fori_loop(1, rows, greet, 0)

    wide_probes = jnp.concatenate(
        [probes_ref[...].astype(f32), jnp.zeros((LANES - nprobe, qcount), f32)], axis=0
    )
    probes = jnp.transpose(wide_probes)
    lane = lax.broadcasted_iota(jnp.int32, (qcount, cold), 1)
    ids = ((lane % rows) * list_dev + lane // rows + hot).astype(f32)
    named = jnp.zeros((qcount, cold), f32)
    for j in range(nprobe):
        named = jnp.where(probes[:, j : j + 1] == ids, 1.0, named)
    below = lax.broadcasted_iota(jnp.int32, (qcount, qcount), 1) < lax.broadcasted_iota(
        jnp.int32, (qcount, qcount), 0
    )
    rank = jnp.dot(below.astype(f32).astype(bf16), named.astype(bf16), preferred_element_type=f32)
    ranks[...] = rank
    order_of = lax.broadcasted_iota(jnp.int32, (qcount, cold), 0).astype(f32) + 1.0
    for r in range(cap):
        held = jnp.where((named > 0) & (rank == float(r)), order_of, 0.0)
        line = jnp.sum(held, axis=0, keepdims=True)
        for l in range(list_dev):
            e = l * cap + r
            table[e : e + 1, :] = line[:, l * rows : (l + 1) * rows]
    block[qcount:depth, 0:rows] = table[0:half, :].astype(bf16)
    block[qcount:depth, rows : 2 * rows] = table[half : 2 * half, :].astype(bf16)
    block[0:qcount, :] = queries_ref[...]
    got[c, 0] = block[...]

    pl.semaphore_wait(barrier, rows - 1)

    def along(da, db):
        return at(da * (1 - c) + db * c, da * c + db * (1 - c), c)

    def push(src, da, db, to_a, to_b):
        slot = ((da - to_a) % side) * side + (db - to_b) % side
        pltpu.make_async_remote_copy(
            src, got.at[c, slot], send_sem, own_sem.at[slot],
            device_id={"row": along(to_a % side, to_b % side)}, device_id_type=MESH,
        ).start()

    def signed(d):
        return d if d <= side // 2 else d - side

    def forward(src, da, db):
        sa, sb = signed(da), signed(db)
        far = side // 2
        if db == 0:
            if sa <= 0 and -sa + 1 <= far:
                push(src, da, db, 1, 0)
            if sa >= 0 and sa + 1 <= far - 1:
                push(src, da, db, -1, 0)
        plus, minus = (far, far - 1) if da % 2 == 0 else (far - 1, far)
        came_plus = db == 0 or sb < 0
        came_minus = db == 0 or (sb > 0 and db != far)
        if came_plus and (0 if db == 0 else -sb) + 1 <= plus:
            push(src, da, db, 0, 1)
        if came_minus and (0 if db == 0 else sb) + 1 <= minus:
            push(src, da, db, 0, -1)

    def to_sibling(src, slot):
        pltpu.make_async_remote_copy(
            src, got.at[c, slot], send_sem, sib_sem.at[slot],
            device_id={"row": at(0, 0, 1 - c)}, device_id_type=MESH,
        ).start()

    def await_block(t, slot, sem):
        here = got.at[t, slot]
        pltpu.make_async_remote_copy(
            here, here, send_sem, sem.at[slot], device_id={"row": me}, device_id_type=MESH
        ).wait_recv()

    order = [(a, b) for a in range(side) for b in range(side)]
    order.sort(key=lambda o: (abs(signed(o[0])) + abs(signed(o[1])), abs(signed(o[1])), o))
    per = LANES // SUB
    step = 4

    choose = (lax.broadcasted_iota(jnp.int32, (rows, LANES), 0) == me).astype(f32).astype(bf16)
    number = lax.broadcasted_iota(jnp.int32, (slots, qcount), 1).astype(f32) + 1.0
    odd = (lax.broadcasted_iota(jnp.int32, (lsize, 2 * LANES), 1) // cap) % 2 == 1

    def slot_of(t, chip):
        return chip[t] * side + chip[1 - t]

    def positions():
        columns = lax.broadcasted_iota(jnp.int32, (qcount, LANES), 1)
        enc = jnp.zeros((qcount, LANES), f32)
        for j in range(nprobe):
            p = probes[:, j : j + 1]
            mine = jnp.sum(jnp.where(p == ids, ranks[...], 0.0), axis=1, keepdims=True)
            n = p.astype(jnp.int32) - hot
            own = n % list_dev
            line = (n // list_dev) * (slots // 2) + (own // 4) * SUB + (own % 2) * cap
            code = jnp.where(n < 0, -1.0, ((line * 2) + (own // 2) % 2).astype(f32) + 2.0 * mine)
            enc = jnp.where(columns == j, code, enc)
        codes = jnp.transpose(enc)[0:nprobe, :].astype(jnp.int32)
        enc_ref[...] = codes
        line_ref[...] = jnp.clip(codes >> 1, 0, out_ref.shape[0] - 1)
        yield

    def hot_work():
        for g in range(hot // SUB):
            for s in range(SUB):
                h = g * SUB + s
                scores = lax.dot_general(hot_ref[h], queries_ref[...], last, preferred_element_type=f32)
                asked = jnp.max((probes_ref[...] == h).astype(f32), axis=0, keepdims=True)
                x[pl.ds(s, lsize, stride=SUB), :] = jnp.where(asked > 0, scores, NEG)
                if s % 4 == 3:
                    yield
            yield from sort_top_128(x, y, mid)
            if g == 0:
                hot_out[...] = y[0 : TOPK * SUB, :]
            else:
                merge_top_128(hot_out, 0, y, 0, hot_out, 0, mid)
            yield

    def batch(b):
        mine = order[b * per : (b + 1) * per]
        for k0 in range(0, per, step):
            yield set(mine[k0 : k0 + step])
            some = [(k, t) for k in range(k0, k0 + step) for t in range(2)]
            for t in range(2):

                @pl.when(c != t)
                def _():
                    for k in range(k0, k0 + step):
                        await_block(t, slot_of(t, mine[k]), sib_sem)

            tables = []
            for k, t in some:
                slot = slot_of(t, mine[k])
                tables += [got[t, slot, qcount:depth, 0:rows], got[t, slot, qcount:depth, rows : 2 * rows]]
            wide = jnp.dot(jnp.concatenate(tables, axis=0), choose, preferred_element_type=f32)
            for n, (k, t) in enumerate(some):
                hits = (wide[n * slots : (n + 1) * slots, :] == number).astype(f32).astype(bf16)
                chosen = jnp.dot(hits, got[t, slot_of(t, mine[k]), 0:qcount, :], preferred_element_type=f32)
                for m in range(pairs):
                    low = t * LANES + k * SUB
                    picked[m, low : low + SUB, :] = chosen[m * SUB : (m + 1) * SUB, :]
        yield
        for m in range(pairs):
            right = picked[m].astype(bf16)
            even_s = lax.dot_general(lists_ref[2 * m], right, last, preferred_element_type=f32)
            odd_s = lax.dot_general(lists_ref[2 * m + 1], right, last, preferred_element_type=f32)
            s = jnp.where(odd, odd_s, even_s)
            for t in range(2):
                x[pl.ds(2 * m + t, lsize, stride=SUB), :] = s[:, t * LANES : (t + 1) * LANES]
            yield
        yield from sort_top_64(x, y)
        for m in range(pairs // 2):
            for t in range(2):
                two = [y[pl.ds(2 * (2 * m + n) + t, FIRST, stride=SUB), :] for n in range(2)]
                sorted_rows = jnp.transpose(jnp.concatenate(two, axis=0))
                back[b * per : (b + 1) * per, t, m * SUB : (m + 1) * SUB, :] = sorted_rows.reshape(per, SUB, LANES)
        yield
        for k in range(per):
            dx, dy = mine[k]
            for t in range(2):

                def give():
                    pltpu.make_async_remote_copy(
                        back.at[b * per + k, t], home, back_sem, ret_sem,
                        device_id={"row": at(dx, dy, t)}, device_id_type=MESH,
                    ).start()

                if (dx, dy) == (0, 0):
                    pl.when(c != t)(give)
                else:
                    give()
            if k % step == step - 1:
                yield

    forward(block, 0, 0)
    to_sibling(block, 0)
    home = out_ref.at[pl.ds(pl.multiple_of(me * (slots // 2), SUB), slots // 2)]

    todo = [positions(), hot_work()] + [batch(b) for b in range(chips // per)]
    passed = {(0, 0)}
    need = [None]

    def advance(count):
        while count and todo:
            if need[0] and not all((a, b) in passed and (b, a) in passed for a, b in need[0]):
                return
            try:
                need[0] = next(todo[0])
                count -= 1
            except StopIteration:
                todo.pop(0)
                need[0] = None

    for da, db in order[1:]:
        slot = da * side + db
        await_block(c, slot, own_sem)
        forward(got.at[c, slot], da, db)
        to_sibling(got.at[c, slot], slot)
        passed.add((da, db))
        advance(1)
    advance(1 << 20)
    home[...] = back[0, c]

    def drain(k, _):
        here = got.at[c, 0]
        pltpu.make_async_remote_copy(
            here, here, send_sem, own_sem.at[0], device_id={"row": me}, device_id_type=MESH
        ).wait_send()
        return 0

    lax.fori_loop(0, 2 * chips - 1, drain, 0)
    to_smem = pltpu.make_async_copy(line_ref, enc_smem, enc_sem)
    to_smem.start()
    to_smem.wait()
    whole = out_ref.at[pl.ds(0, (rows - 1) * (slots // 2))]
    done = pltpu.make_async_remote_copy(
        whole, whole, back_sem, ret_sem, device_id={"row": me}, device_id_type=MESH
    )
    done.wait_send()
    done.wait_recv()

    assert out_ref.shape[0] & (out_ref.shape[0] - 1) == 0

    def gather(j, _):
        def one(q, _):
            line = enc_smem[j, q] & (out_ref.shape[0] - 1)
            buf[pl.ds(j * qcount + q, 1), :] = out_ref[pl.ds(line, 1), :]
            return 0

        lax.fori_loop(0, qcount, one, 0, unroll=16)
        return 0

    lax.fori_loop(0, nprobe, gather, 0)
    enc = enc_ref[...]
    for j in range(nprobe):
        both = jnp.transpose(buf[j * qcount : (j + 1) * qcount, :])
        flat = jnp.where(enc[j : j + 1, :] % 2 == 0, both[0:FIRST, :], both[FIRST : 2 * FIRST, :])
        flat = jnp.where(enc[j : j + 1, :] < 0, NEG, flat)
        lists_a[pl.ds((j // SUB) * FIRST * SUB + j % SUB, FIRST, stride=SUB), :] = flat

    least = jnp.maximum(lists_a[row(FIRST - 1, 0), :], lists_a[row(2 * FIRST - 1, 0), :])
    for shift in (4, 2, 1):
        least = jnp.maximum(least, pltpu.roll(least, shift, 0))
    count = jnp.zeros((SUB, LANES), f32)
    for k in range(TOPK):
        count += (lists_a[row(k, 0), :] >= least).astype(f32) + (hot_out[row(k, 0), :] >= least).astype(f32)
    for shift in (4, 2, 1):
        count += pltpu.roll(count, shift, 0)
    note[0] = (count < float(TOPK)).astype(f32)
    merge_full_64(lists_a, lists_b, 1)

    def tell(number, src, dx, dy, core, dst, sem):
        pltpu.make_async_remote_copy(
            src, dst.at[number], note_sem, sem, device_id={"row": at(dx, dy, core)}, device_id_type=MESH
        ).start()

    def heard(dst, sem):
        pltpu.make_async_remote_copy(dst, dst, note_sem, sem, device_id={"row": me}, device_id_type=MESH).wait_recv()

    near = [(dx, t) for dx in range(side) for t in range(2)]
    for dx, t in near[1:]:
        tell(2 * dx + t - 1, note.at[0], dx, 0, (c + t) % 2, notes_x, nx_sem)
    merge_top_128(lists_b, 0, hot_out, 0, lists_a, 0, mid)
    merge_top_128(lists_a, 0, lists_a, 0, lists_b, 0, mid, 4)
    heard(notes_x, nx_sem)
    note[1] = jnp.maximum(note[0], jnp.max(notes_x[...], axis=0))
    merge_top_128(lists_b, 0, lists_b, 0, lists_a, 0, mid, 2)
    for dy in range(1, side):
        tell(dy - 1, note.at[1], 0, dy, c, notes_y, ny_sem)
    merge_top_128(lists_a, 0, lists_a, 0, lists_b, 0, mid, 1)
    best_ref[...] = jnp.transpose(lists_b[pl.ds(0, TOPK, stride=SUB), :])
    heard(notes_y, ny_sem)
    flag_ref[0, 0] = jnp.max(jnp.maximum(note[1], jnp.max(notes_y[...], axis=0))).astype(jnp.int32)
    for sent in (notes_x, notes_y):
        pltpu.make_async_remote_copy(
            sent, sent, note_sem, nx_sem, device_id={"row": me}, device_id_type=MESH
        ).wait_send()


def slow_prepare(rows, list_dev, hot, cap, probes_ref, queries_ref, block_ref, enc_ref, table):
    qcount, nprobe = probes_ref.shape
    cold = rows * list_dev
    lane = lax.broadcasted_iota(jnp.int32, (qcount, cold), 1)
    ids = (lane % rows) * list_dev + lane // rows + hot
    probes = probes_ref[...]
    named = jnp.zeros((qcount, cold), jnp.float32)
    for j in range(nprobe):
        named = jnp.where(probes[:, j : j + 1] == ids, 1.0, named)
    below = lax.broadcasted_iota(jnp.int32, (qcount, qcount), 1) < lax.broadcasted_iota(
        jnp.int32, (qcount, qcount), 0
    )
    rank = jnp.dot(
        below.astype(jnp.float32).astype(jnp.bfloat16),
        named.astype(jnp.bfloat16),
        preferred_element_type=jnp.float32,
    )
    number = lax.broadcasted_iota(jnp.int32, (qcount, cold), 0).astype(jnp.float32) + 1.0
    for r in range(cap):
        held = jnp.where((named > 0) & (rank == float(r)), number, 0.0)
        line = jnp.sum(held, axis=0, keepdims=True)
        for l in range(list_dev):
            e = l * cap + r
            table[e : e + 1, :] = line[:, l * rows : (l + 1) * rows]
    half = list_dev * cap // 2
    block_ref[0:qcount, :] = queries_ref[...]
    block_ref[qcount : qcount + half, 0:rows] = table[0:half, :].astype(jnp.bfloat16)
    block_ref[qcount : qcount + half, rows : 2 * rows] = table[half : 2 * half, :].astype(
        jnp.bfloat16
    )
    columns = lax.broadcasted_iota(jnp.int32, (qcount, LANES), 1)
    enc = jnp.zeros((qcount, LANES), jnp.float32)
    for j in range(nprobe):
        p = probes[:, j : j + 1]
        mine = jnp.sum(jnp.where(p == ids, rank, 0.0), axis=1, keepdims=True)
        pf = p.astype(jnp.float32)
        code = jnp.where(p < hot, -1.0 - pf, (pf - hot) * cap + mine)
        enc = jnp.where(columns == j, code, enc)
    enc_ref[...] = jnp.transpose(enc)[0:nprobe, :].astype(jnp.int32)


def slow_exchange(rows, side, list_dev, cap, block_ref, lists_ref, out_ref, got, picked, x, y, mid, back,
             send_sem, own_sem, sib_sem, back_sem, ret_sem):
    me = lax.axis_index("row")
    mx, my, c = me // (2 * side), (me // 2) % side, me % 2
    chips = side * side
    depth = block_ref.shape[0]
    half = list_dev * cap // 2
    qcount = depth - half
    slots = list_dev * cap
    pairs = list_dev // 2

    def at(dx, dy, core):
        return (((mx + dx) % side) * side + (my + dy) % side) * 2 + core

    barrier = pltpu.get_barrier_semaphore()

    def greet(k, _):
        pl.semaphore_signal(barrier, 1, device_id={"row": (me + k) % rows}, device_id_type=MESH)
        return 0

    lax.fori_loop(1, rows, greet, 0)
    pl.semaphore_wait(barrier, rows - 1)

    def along(da, db):
        return at(da * (1 - c) + db * c, da * c + db * (1 - c), c)

    def push(src, da, db, to_a, to_b):
        slot = ((da - to_a) % side) * side + (db - to_b) % side
        pltpu.make_async_remote_copy(
            src, got.at[c, slot], send_sem, own_sem.at[slot],
            device_id={"row": along(to_a % side, to_b % side)}, device_id_type=MESH,
        ).start()

    def signed(d):
        return d if d <= side // 2 else d - side

    def forward(src, da, db):
        sa, sb = signed(da), signed(db)
        far = side // 2
        if db == 0:
            if sa <= 0 and -sa + 1 <= far and da != far:
                push(src, da, db, 1, 0)
            if sa >= 0 and sa + 1 <= far - 1:
                push(src, da, db, -1, 0)
        plus, minus = (far, far - 1) if da % 2 == 0 else (far - 1, far)
        came_plus = db == 0 or sb < 0
        came_minus = db == 0 or (sb > 0 and db != far)
        if came_plus and (0 if db == 0 else -sb) + 1 <= plus:
            push(src, da, db, 0, 1)
        if came_minus and (0 if db == 0 else sb) + 1 <= minus:
            push(src, da, db, 0, -1)

    def to_sibling(src, slot):
        pltpu.make_async_remote_copy(
            src, got.at[c, slot], send_sem, sib_sem.at[slot],
            device_id={"row": at(0, 0, 1 - c)}, device_id_type=MESH,
        ).start()

    forward(block_ref, 0, 0)
    to_sibling(block_ref, 0)
    got[c, 0] = block_ref[...]
    order = [(a, b) for a in range(side) for b in range(side) if (a, b) != (0, 0)]
    order.sort(key=lambda o: (abs(signed(o[0])) + abs(signed(o[1])), abs(signed(o[1])), o))
    for da, db in order:
        slot = da * side + db
        here = got.at[c, slot]
        pltpu.make_async_remote_copy(
            here, here, send_sem, own_sem.at[slot], device_id={"row": me}, device_id_type=MESH
        ).wait_recv()
        forward(here, da, db)
        to_sibling(here, slot)

    share = chips // (LANES // SUB)
    per = chips // share
    choose = (lax.broadcasted_iota(jnp.int32, (rows, LANES), 0) == me).astype(jnp.float32).astype(jnp.bfloat16)
    number = lax.broadcasted_iota(jnp.int32, (slots, qcount), 1).astype(jnp.float32) + 1.0
    odd = (lax.broadcasted_iota(jnp.int32, (lists_ref.shape[1], 2 * LANES), 1) // cap) % 2 == 1

    def batch(b, _):
        def take(k, _):
            i = b * per + k
            for t in range(2):
                slot = i if t == 0 else (i % side) * side + i // side
                here = got.at[t, slot]

                @pl.when((c != t))
                def _():
                    pltpu.make_async_remote_copy(
                        here, here, send_sem, sib_sem.at[slot], device_id={"row": me}, device_id_type=MESH
                    ).wait_recv()

                table = jnp.concatenate(
                    [got[t, slot, qcount:depth, 0:rows], got[t, slot, qcount:depth, rows : 2 * rows]], axis=0
                )
                wide = jnp.dot(table, choose, preferred_element_type=jnp.float32)
                hits = (wide == number).astype(jnp.float32).astype(jnp.bfloat16)
                chosen = jnp.dot(hits, got[t, slot, 0:qcount, :], preferred_element_type=jnp.float32)
                for m in range(pairs):
                    picked[m, pl.ds(pl.multiple_of(t * LANES + k * SUB, SUB), SUB), :] = chosen[
                        m * SUB : (m + 1) * SUB, :
                    ]
            return 0

        lax.fori_loop(0, per, take, 0)

        for m in range(pairs):
            right = picked[m].astype(jnp.bfloat16)
            dims = (((1,), (1,)), ((), ()))
            even_s = lax.dot_general(lists_ref[2 * m], right, dims, preferred_element_type=jnp.float32)
            odd_s = lax.dot_general(lists_ref[2 * m + 1], right, dims, preferred_element_type=jnp.float32)
            s = jnp.where(odd, odd_s, even_s)
            for t in range(2):
                x[pl.ds(2 * m + t, s.shape[0], stride=SUB), :] = s[:, t * LANES : (t + 1) * LANES]
        run(sort_top_128(x, y, mid))
        for m in range(pairs):
            for t in range(2):
                sorted_rows = jnp.transpose(y[pl.ds(2 * m + t, TOPK, stride=SUB), :])
                back[pl.ds(b * per, per), t, m * SUB : (m + 1) * SUB, :] = sorted_rows.reshape(per, SUB, TOPK)

        def give(k, _):
            i = b * per + k
            for t in range(2):

                @pl.when((i != 0) | (c != t))
                def _():
                    pltpu.make_async_remote_copy(
                        back.at[i, t], out_ref.at[me], back_sem, ret_sem,
                        device_id={"row": at(i // side, i % side, t)}, device_id_type=MESH,
                    ).start()
            return 0

        lax.fori_loop(0, per, give, 0)
        return 0

    lax.fori_loop(0, share, batch, 0)
    out_ref[me] = back[0, c]

    def drain(k, _):
        here = got.at[c, 0]
        pltpu.make_async_remote_copy(
            here, here, send_sem, own_sem.at[0], device_id={"row": me}, device_id_type=MESH
        ).wait_send()
        return 0

    lax.fori_loop(0, 2 * chips - 1, drain, 0)
    whole = out_ref.at[pl.ds(0, rows - 1)]
    done = pltpu.make_async_remote_copy(
        whole, whole, back_sem, ret_sem, device_id={"row": me}, device_id_type=MESH
    )
    done.wait_send()
    done.wait_recv()


def slow_finish(enc_smem, enc_ref, rows_ref, queries_ref, hot_ref, out_ref, buf, x, y, mid, lists_a, lists_b):
    nprobe, qcount = enc_ref.shape
    hot = hot_ref.shape[0]
    enc = enc_ref[...]

    def gather(j, _):
        def one(q, _):
            at = jnp.maximum(enc_smem[j, q], 0)
            buf[pl.ds(j * qcount + q, 1), :] = rows_ref[pl.ds(at, 1), :]
            return 0

        lax.fori_loop(0, qcount, one, 0, unroll=16)
        return 0

    lax.fori_loop(0, nprobe, gather, 0)
    for j in range(nprobe):
        dst = lists_a if j < SUB else lists_b
        flat = jnp.transpose(buf[j * qcount : (j + 1) * qcount, :])
        flat = jnp.where(enc[j : j + 1, :] < 0, NEG, flat)
        dst[pl.ds(j % SUB, TOPK, stride=SUB), :] = flat
    merge_top_128(lists_a, 0, lists_b, 0, lists_a, 0, mid)
    for g in range(hot // SUB):
        for s in range(SUB):
            h = g * SUB + s
            scores = lax.dot_general(
                hot_ref[h], queries_ref[...], (((1,), (1,)), ((), ())), preferred_element_type=jnp.float32
            )
            asked = jnp.max((enc == -1 - h).astype(jnp.float32), axis=0, keepdims=True)
            x[pl.ds(s, scores.shape[0], stride=SUB), :] = jnp.where(asked > 0, scores, NEG)
        run(sort_top_128(x, y, mid))
        merge_top_128(lists_a, 0, y, 0, lists_a, 0, mid)
    for shift in (4, 2, 1):
        merge_top_128(lists_a, 0, lists_a, 0, lists_b, 0, mid, shift)
        lists_a, lists_b = lists_b, lists_a
    out_ref[...] = jnp.transpose(lists_a[pl.ds(0, TOPK, stride=SUB), :])


def shards(queries, probes, hot_lists, cold_lists):
    rows = lax.axis_size("row")
    side = math.isqrt(rows // 2)
    qcount, nprobe = probes.shape
    width = queries.shape[1]
    list_dev, lsize = cold_lists.shape[0], cold_lists.shape[1]
    hot = hot_lists.shape[0]
    cap = 2 * ((qcount * nprobe + list_dev * rows - 1) // (list_dev * rows))
    slots = list_dev * cap
    depth = qcount + slots // 2
    vmem = pl.BlockSpec(memory_space=pltpu.VMEM)
    limit = 60 * 2**20
    f32 = jnp.float32
    column = pltpu.VMEM((lsize * SUB, LANES), f32)
    small = pltpu.VMEM((TOPK * SUB, LANES), f32)

    best, flag = pl.pallas_call(
        functools.partial(exchange, rows, side, cap),
        out_shape=(
            jax.ShapeDtypeStruct((qcount, TOPK), f32),
            jax.ShapeDtypeStruct((1, 1), jnp.int32),
        ),
        in_specs=[vmem] * 4,
        out_specs=(vmem, pl.BlockSpec(memory_space=pltpu.SMEM)),
        scratch_shapes=[
            pltpu.VMEM((depth, width), jnp.bfloat16),
            pltpu.VMEM((slots, rows), f32),
            pltpu.VMEM((qcount, rows * list_dev), f32),
            pltpu.VMEM((2, side * side, depth, width), jnp.bfloat16),
            pltpu.VMEM((list_dev // 2, 2 * LANES, width), f32),
            column,
            column,
            small,
            pltpu.VMEM((side * side, 2, slots // 2, LANES), f32),
            pltpu.VMEM((rows * slots // 2, LANES), f32),
            pltpu.VMEM((nprobe, qcount), jnp.int32),
            pltpu.VMEM((nprobe, qcount), jnp.int32),
            pltpu.SMEM((nprobe, qcount), jnp.int32),
            small,
            pltpu.VMEM((nprobe * qcount, LANES), f32),
            small,
            small,
            pltpu.VMEM((2, SUB, LANES), f32),
            pltpu.VMEM((2 * side - 1, SUB, LANES), f32),
            pltpu.VMEM((side - 1, SUB, LANES), f32),
            pltpu.SemaphoreType.DMA,
            pltpu.SemaphoreType.DMA((side * side,)),
            pltpu.SemaphoreType.DMA((side * side,)),
            pltpu.SemaphoreType.DMA,
            pltpu.SemaphoreType.DMA,
            pltpu.SemaphoreType.DMA,
            pltpu.SemaphoreType.DMA,
            pltpu.SemaphoreType.DMA,
            pltpu.SemaphoreType.DMA,
        ],
        compiler_params=pltpu.CompilerParams(collective_id=0, has_side_effects=True, vmem_limit_bytes=limit),
    )(probes.T, queries, cold_lists, hot_lists)

    def full(best, queries, probes, hot_lists, cold_lists):
        block, enc = pl.pallas_call(
            functools.partial(slow_prepare, rows, list_dev, hot, cap),
            out_shape=(
                jax.ShapeDtypeStruct((depth, width), jnp.bfloat16),
                jax.ShapeDtypeStruct((nprobe, qcount), jnp.int32),
            ),
            in_specs=[vmem] * 2,
            out_specs=(vmem, vmem),
            scratch_shapes=[pltpu.VMEM((slots, rows), f32)],
            compiler_params=pltpu.CompilerParams(vmem_limit_bytes=limit),
        )(probes, queries)
        returned = pl.pallas_call(
            functools.partial(slow_exchange, rows, side, list_dev, cap),
            out_shape=jax.ShapeDtypeStruct((rows, slots, TOPK), f32),
            in_specs=[vmem] * 2,
            out_specs=vmem,
            scratch_shapes=[
                pltpu.VMEM((2, side * side, depth, width), jnp.bfloat16),
                pltpu.VMEM((list_dev // 2, 2 * LANES, width), f32),
                column,
                column,
                small,
                pltpu.VMEM((side * side, 2, slots, TOPK), f32),
                pltpu.SemaphoreType.DMA,
                pltpu.SemaphoreType.DMA((side * side,)),
                pltpu.SemaphoreType.DMA((side * side,)),
                pltpu.SemaphoreType.DMA,
                pltpu.SemaphoreType.DMA,
            ],
            compiler_params=pltpu.CompilerParams(collective_id=1, has_side_effects=True, vmem_limit_bytes=limit),
        )(block, cold_lists)
        return pl.pallas_call(
            slow_finish,
            out_shape=jax.ShapeDtypeStruct((qcount, TOPK), f32),
            in_specs=[pl.BlockSpec(memory_space=pltpu.SMEM)] + [vmem] * 4,
            out_specs=vmem,
            scratch_shapes=[pltpu.VMEM((nprobe * qcount, TOPK), f32), column, column, small, small, small],
            compiler_params=pltpu.CompilerParams(vmem_limit_bytes=limit),
        )(enc, enc, returned.reshape(rows * slots, TOPK), queries, hot_lists)

    return lax.cond(
        flag[0, 0] > 0, full, lambda best, *_: best, best, queries, probes, hot_lists, cold_lists
    )


def solution(mesh):
    placed = (
        P(("tenant", "row"), None),
        P(("tenant", "row"), None),
        P("tenant", None, None),
        P(("tenant", "row"), None, None),
    )
    return jax.shard_map(
        shards, mesh=mesh, in_specs=placed, out_specs=P(("tenant", "row"), None), check_vma=False
    )
```

```python
import functools
import math

import jax
import jax.numpy as jnp
from jax import lax
from jax.experimental import pallas as pl
from jax.experimental.pallas import tpu as pltpu
from jax.sharding import PartitionSpec as P

MESH = pl.DeviceIdType.MESH
TOPK = 128
FIRST = 64
LANES = 128
SUB = 8
NEG = float("-inf")


def odd_even(n):
    pairs = []

    def merge(lo, hi, step):
        jump = step * 2
        if jump < hi - lo:
            merge(lo, hi, jump)
            merge(lo + step, hi, jump)
            pairs.extend((i, i + step) for i in range(lo + step, hi - step, jump))
        else:
            pairs.append((lo, lo + step))

    def sort(lo, hi):
        if hi - lo >= 1:
            mid = lo + (hi - lo) // 2
            sort(lo, mid)
            sort(mid + 1, hi)
            merge(lo, hi, 1)

    sort(0, n - 1)
    return pairs


def bitonic(values, distances):
    values = list(values)
    for d in distances:
        for i in range(len(values)):
            if i & d == 0:
                a, b = values[i], values[i + d]
                values[i], values[i + d] = jnp.maximum(a, b), jnp.minimum(a, b)
    return values


def row(base, i):
    at = (base + i) * SUB
    return pl.ds(at if isinstance(at, int) else pl.multiple_of(at, SUB), SUB)


def sort_groups(ref, start, stop, n=32):
    pairs = odd_even(n)

    def body(g, _):
        v = [ref[row(g * n, i), :] for i in range(n)]
        for a, b in pairs:
            v[a], v[b] = jnp.maximum(v[a], v[b]), jnp.minimum(v[a], v[b])
        for i in range(n):
            ref[row(g * n, i), :] = v[i]
        return 0

    lax.fori_loop(start, stop, body, 0)


def merge_full_32(src, dst, count):
    def body(g, _):
        base = g * 64
        for pick, at in ((jnp.maximum, 0), (jnp.minimum, 32)):
            v = [pick(src[row(base, i), :], src[row(base + 32, 31 - i), :]) for i in range(32)]
            v = bitonic(v, (16, 8, 4, 2, 1))
            for i in range(32):
                dst[row(base + at, i), :] = v[i]
        return 0

    lax.fori_loop(0, count, body, 0)


def half_64(src, a, b, outer, inner):
    v = []
    for i in range(32):
        low = outer(src[row(a, i), :], src[row(b, 63 - i), :])
        high = outer(src[row(a, i + 32), :], src[row(b, 31 - i), :])
        v.append(inner(low, high))
    return bitonic(v, (16, 8, 4, 2, 1))


def merge_full_64(src, dst, count):
    def body(g, _):
        base = g * 128
        at = 0
        for outer in (jnp.maximum, jnp.minimum):
            for inner in (jnp.maximum, jnp.minimum):
                v = half_64(src, base, base + 64, outer, inner)
                for i in range(32):
                    dst[row(base + at, i), :] = v[i]
                at += 32
        return 0

    lax.fori_loop(0, count, body, 0)


def merge_top_128(a, a0, b, b0, dst, d0, mid, shift=0):
    def first(g, _):
        v = []
        for k in range(8):
            other = b[row(b0 + 127 - g - 16 * k, 0), :]
            if shift:
                other = pltpu.roll(other, shift, 0)
            v.append(jnp.maximum(a[row(a0 + g + 16 * k, 0), :], other))
        v = bitonic(v, (4, 2, 1))
        for k in range(8):
            mid[row(g + 16 * k, 0), :] = v[k]
        return 0

    lax.fori_loop(0, 16, first, 0, unroll=2)

    def second(g, _):
        v = bitonic([mid[row(g * 16, i), :] for i in range(16)], (8, 4, 2, 1))
        for i in range(16):
            dst[row(d0 + g * 16, i), :] = v[i]
        return 0

    lax.fori_loop(0, 8, second, 0, unroll=2)


def sort_top_128(x, y, mid):
    sort_groups(x, 0, 4)
    yield
    sort_groups(x, 4, 8)
    yield
    merge_full_32(x, y, 4)
    yield
    merge_full_64(y, x, 2)
    yield
    merge_top_128(x, 0, x, 128, y, 0, mid)
    yield


def sort_top_64(x, y):
    sort_groups(x, 0, 4)
    yield
    sort_groups(x, 4, 8)
    yield
    merge_full_32(x, y, 4)
    yield
    for src, dst, count in ((y, x, 2), (x, y, 1)):
        for g in range(count):
            for n, inner in enumerate((jnp.maximum, jnp.minimum)):
                v = half_64(src, g * 128, g * 128 + 64, jnp.maximum, inner)
                for i in range(32):
                    dst[row(g * 64 + n * 32, i), :] = v[i]
        yield


def run(pieces):
    for _ in pieces:
        pass


def exchange(rows, side, cap, probes_ref, queries_ref, lists_ref, hot_ref, best_ref, flag_ref, block, table, ranks,
             got, picked, x, y, mid, back, out_ref, enc_ref, line_ref, enc_smem, hot_out, buf, lists_a, lists_b, note, notes_x, notes_y,
             send_sem, own_sem, sib_sem, back_sem, ret_sem, enc_sem, note_sem, nx_sem, ny_sem):
    me = lax.axis_index("row")
    mx, my, c = me // (2 * side), (me // 2) % side, me % 2
    chips = side * side
    list_dev, lsize = lists_ref.shape[0], lists_ref.shape[1]
    hot = hot_ref.shape[0]
    nprobe, qcount = probes_ref.shape
    slots = list_dev * cap
    half = slots // 2
    depth = qcount + half
    pairs = list_dev // 2
    cold = rows * list_dev
    f32, bf16 = jnp.float32, jnp.bfloat16
    last = (((1,), (1,)), ((), ()))

    def at(dx, dy, core):
        return (((mx + dx) % side) * side + (my + dy) % side) * 2 + core

    barrier = pltpu.get_barrier_semaphore()

    def greet(k, _):
        pl.semaphore_signal(barrier, 1, device_id={"row": (me + k) % rows}, device_id_type=MESH)
        return 0

    lax.fori_loop(1, rows, greet, 0)

    wide_probes = jnp.concatenate(
        [probes_ref[...].astype(f32), jnp.zeros((LANES - nprobe, qcount), f32)], axis=0
    )
    probes = jnp.transpose(wide_probes)
    lane = lax.broadcasted_iota(jnp.int32, (qcount, cold), 1)
    ids = ((lane % rows) * list_dev + lane // rows + hot).astype(f32)
    named = jnp.zeros((qcount, cold), f32)
    for j in range(nprobe):
        named = jnp.where(probes[:, j : j + 1] == ids, 1.0, named)
    below = lax.broadcasted_iota(jnp.int32, (qcount, qcount), 1) < lax.broadcasted_iota(
        jnp.int32, (qcount, qcount), 0
    )
    rank = jnp.dot(below.astype(f32).astype(bf16), named.astype(bf16), preferred_element_type=f32)
    ranks[...] = rank
    order_of = lax.broadcasted_iota(jnp.int32, (qcount, cold), 0).astype(f32) + 1.0
    for r in range(cap):
        held = jnp.where((named > 0) & (rank == float(r)), order_of, 0.0)
        line = jnp.sum(held, axis=0, keepdims=True)
        for l in range(list_dev):
            e = l * cap + r
            table[e : e + 1, :] = line[:, l * rows : (l + 1) * rows]
    block[qcount:depth, 0:rows] = table[0:half, :].astype(bf16)
    block[qcount:depth, rows : 2 * rows] = table[half : 2 * half, :].astype(bf16)
    block[0:qcount, :] = queries_ref[...]
    got[c, 0] = block[...]

    pl.semaphore_wait(barrier, rows - 1)

    def along(da, db):
        return at(da * (1 - c) + db * c, da * c + db * (1 - c), c)

    def push(src, da, db, to_a, to_b):
        slot = ((da - to_a) % side) * side + (db - to_b) % side
        pltpu.make_async_remote_copy(
            src, got.at[c, slot], send_sem, own_sem.at[slot],
            device_id={"row": along(to_a % side, to_b % side)}, device_id_type=MESH,
        ).start()

    def signed(d):
        return d if d <= side // 2 else d - side

    def forward(src, da, db):
        sa, sb = signed(da), signed(db)
        far = side // 2
        if db == 0:
            if sa <= 0 and -sa + 1 <= far:
                push(src, da, db, 1, 0)
            if sa >= 0 and sa + 1 <= far - 1:
                push(src, da, db, -1, 0)
        plus, minus = (far, far - 1) if da % 2 == 0 else (far - 1, far)
        came_plus = db == 0 or sb < 0
        came_minus = db == 0 or (sb > 0 and db != far)
        if came_plus and (0 if db == 0 else -sb) + 1 <= plus:
            push(src, da, db, 0, 1)
        if came_minus and (0 if db == 0 else sb) + 1 <= minus:
            push(src, da, db, 0, -1)

    def to_sibling(src, slot):
        pltpu.make_async_remote_copy(
            src, got.at[c, slot], send_sem, sib_sem.at[slot],
            device_id={"row": at(0, 0, 1 - c)}, device_id_type=MESH,
        ).start()

    def await_block(t, slot, sem):
        here = got.at[t, slot]
        pltpu.make_async_remote_copy(
            here, here, send_sem, sem.at[slot], device_id={"row": me}, device_id_type=MESH
        ).wait_recv()

    order = [(a, b) for a in range(side) for b in range(side)]
    order.sort(key=lambda o: (abs(signed(o[0])) + abs(signed(o[1])), abs(signed(o[1])), o))
    per = LANES // SUB
    step = 4

    choose = (lax.broadcasted_iota(jnp.int32, (rows, LANES), 0) == me).astype(f32).astype(bf16)
    number = lax.broadcasted_iota(jnp.int32, (slots, qcount), 1).astype(f32) + 1.0
    odd = (lax.broadcasted_iota(jnp.int32, (lsize, 2 * LANES), 1) // cap) % 2 == 1

    def slot_of(t, chip):
        return chip[t] * side + chip[1 - t]

    def positions():
        columns = lax.broadcasted_iota(jnp.int32, (qcount, LANES), 1)
        enc = jnp.zeros((qcount, LANES), f32)
        for j in range(nprobe):
            p = probes[:, j : j + 1]
            mine = jnp.sum(jnp.where(p == ids, ranks[...], 0.0), axis=1, keepdims=True)
            n = p.astype(jnp.int32) - hot
            own = n % list_dev
            line = (n // list_dev) * (slots // 2) + (own // 4) * SUB + (own % 2) * cap
            code = jnp.where(n < 0, -1.0, ((line * 2) + (own // 2) % 2).astype(f32) + 2.0 * mine)
            enc = jnp.where(columns == j, code, enc)
        codes = jnp.transpose(enc)[0:nprobe, :].astype(jnp.int32)
        enc_ref[...] = codes
        line_ref[...] = jnp.clip(codes >> 1, 0, out_ref.shape[0] - 1)
        yield

    def hot_work():
        for g in range(hot // SUB):
            for s in range(SUB):
                h = g * SUB + s
                scores = lax.dot_general(hot_ref[h], queries_ref[...], last, preferred_element_type=f32)
                asked = jnp.max((probes_ref[...] == h).astype(f32), axis=0, keepdims=True)
                x[pl.ds(s, lsize, stride=SUB), :] = jnp.where(asked > 0, scores, NEG)
                if s % 4 == 3:
                    yield
            yield from sort_top_128(x, y, mid)
            if g == 0:
                hot_out[...] = y[0 : TOPK * SUB, :]
            else:
                merge_top_128(hot_out, 0, y, 0, hot_out, 0, mid)
            yield

    def batch(b):
        mine = order[b * per : (b + 1) * per]
        for k0 in range(0, per, step):
            yield set(mine[k0 : k0 + step])
            some = [(k, t) for k in range(k0, k0 + step) for t in range(2)]
            for t in range(2):

                @pl.when(c != t)
                def _():
                    for k in range(k0, k0 + step):
                        await_block(t, slot_of(t, mine[k]), sib_sem)

            tables = []
            for k, t in some:
                slot = slot_of(t, mine[k])
                tables += [got[t, slot, qcount:depth, 0:rows], got[t, slot, qcount:depth, rows : 2 * rows]]
            wide = jnp.dot(jnp.concatenate(tables, axis=0), choose, preferred_element_type=f32)
            for n, (k, t) in enumerate(some):
                hits = (wide[n * slots : (n + 1) * slots, :] == number).astype(f32).astype(bf16)
                chosen = jnp.dot(hits, got[t, slot_of(t, mine[k]), 0:qcount, :], preferred_element_type=f32)
                for m in range(pairs):
                    low = t * LANES + k * SUB
                    picked[m, low : low + SUB, :] = chosen[m * SUB : (m + 1) * SUB, :]
        yield
        for m in range(pairs):
            right = picked[m].astype(bf16)
            even_s = lax.dot_general(lists_ref[2 * m], right, last, preferred_element_type=f32)
            odd_s = lax.dot_general(lists_ref[2 * m + 1], right, last, preferred_element_type=f32)
            s = jnp.where(odd, odd_s, even_s)
            for t in range(2):
                x[pl.ds(2 * m + t, lsize, stride=SUB), :] = s[:, t * LANES : (t + 1) * LANES]
            yield
        yield from sort_top_64(x, y)
        for m in range(pairs // 2):
            for t in range(2):
                two = [y[pl.ds(2 * (2 * m + n) + t, FIRST, stride=SUB), :] for n in range(2)]
                sorted_rows = jnp.transpose(jnp.concatenate(two, axis=0))
                back[b * per : (b + 1) * per, t, m * SUB : (m + 1) * SUB, :] = sorted_rows.reshape(per, SUB, LANES)
        yield
        for k in range(per):
            dx, dy = mine[k]
            for t in range(2):

                def give():
                    pltpu.make_async_remote_copy(
                        back.at[b * per + k, t], home, back_sem, ret_sem,
                        device_id={"row": at(dx, dy, t)}, device_id_type=MESH,
                    ).start()

                if (dx, dy) == (0, 0):
                    pl.when(c != t)(give)
                else:
                    give()
            if k % step == step - 1:
                yield

    forward(block, 0, 0)
    to_sibling(block, 0)
    home = out_ref.at[pl.ds(pl.multiple_of(me * (slots // 2), SUB), slots // 2)]

    todo = [positions(), hot_work()] + [batch(b) for b in range(chips // per)]
    passed = {(0, 0)}
    need = [None]

    def advance(count):
        while count and todo:
            if need[0] and not all((a, b) in passed and (b, a) in passed for a, b in need[0]):
                return
            try:
                need[0] = next(todo[0])
                count -= 1
            except StopIteration:
                todo.pop(0)
                need[0] = None

    for da, db in order[1:]:
        slot = da * side + db
        await_block(c, slot, own_sem)
        forward(got.at[c, slot], da, db)
        to_sibling(got.at[c, slot], slot)
        passed.add((da, db))
        advance(1 if len(passed) < 14 else 2)
    advance(1 << 20)
    home[...] = back[0, c]

    def drain(k, _):
        here = got.at[c, 0]
        pltpu.make_async_remote_copy(
            here, here, send_sem, own_sem.at[0], device_id={"row": me}, device_id_type=MESH
        ).wait_send()
        return 0

    lax.fori_loop(0, 2 * chips - 1, drain, 0)
    to_smem = pltpu.make_async_copy(line_ref, enc_smem, enc_sem)
    to_smem.start()
    to_smem.wait()
    whole = out_ref.at[pl.ds(0, (rows - 1) * (slots // 2))]
    done = pltpu.make_async_remote_copy(
        whole, whole, back_sem, ret_sem, device_id={"row": me}, device_id_type=MESH
    )
    done.wait_send()
    done.wait_recv()

    assert out_ref.shape[0] & (out_ref.shape[0] - 1) == 0

    def gather(j, _):
        def one(q, _):
            line = enc_smem[j, q] & (out_ref.shape[0] - 1)
            buf[pl.ds(j * qcount + q, 1), :] = out_ref[pl.ds(line, 1), :]
            return 0

        lax.fori_loop(0, qcount, one, 0, unroll=16)
        return 0

    lax.fori_loop(0, nprobe, gather, 0)
    enc = enc_ref[...]
    for j in range(nprobe):
        both = jnp.transpose(buf[j * qcount : (j + 1) * qcount, :])
        flat = jnp.where(enc[j : j + 1, :] % 2 == 0, both[0:FIRST, :], both[FIRST : 2 * FIRST, :])
        flat = jnp.where(enc[j : j + 1, :] < 0, NEG, flat)
        lists_a[pl.ds((j // SUB) * FIRST * SUB + j % SUB, FIRST, stride=SUB), :] = flat

    least = jnp.maximum(lists_a[row(FIRST - 1, 0), :], lists_a[row(2 * FIRST - 1, 0), :])
    for shift in (4, 2, 1):
        least = jnp.maximum(least, pltpu.roll(least, shift, 0))
    count = jnp.zeros((SUB, LANES), f32)
    for k in range(TOPK):
        count += (lists_a[row(k, 0), :] >= least).astype(f32) + (hot_out[row(k, 0), :] >= least).astype(f32)
    for shift in (4, 2, 1):
        count += pltpu.roll(count, shift, 0)
    note[0] = (count < float(TOPK)).astype(f32)
    merge_full_64(lists_a, lists_b, 1)

    def tell(number, src, dx, dy, core, dst, sem):
        pltpu.make_async_remote_copy(
            src, dst.at[number], note_sem, sem, device_id={"row": at(dx, dy, core)}, device_id_type=MESH
        ).start()

    def heard(dst, sem):
        pltpu.make_async_remote_copy(dst, dst, note_sem, sem, device_id={"row": me}, device_id_type=MESH).wait_recv()

    near = [(dx, t) for dx in range(side) for t in range(2)]
    for dx, t in near[1:]:
        tell(2 * dx + t - 1, note.at[0], dx, 0, (c + t) % 2, notes_x, nx_sem)
    merge_top_128(lists_b, 0, hot_out, 0, lists_a, 0, mid)
    merge_top_128(lists_a, 0, lists_a, 0, lists_b, 0, mid, 4)
    heard(notes_x, nx_sem)
    note[1] = jnp.maximum(note[0], jnp.max(notes_x[...], axis=0))
    merge_top_128(lists_b, 0, lists_b, 0, lists_a, 0, mid, 2)
    for dy in range(1, side):
        tell(dy - 1, note.at[1], 0, dy, c, notes_y, ny_sem)
    merge_top_128(lists_a, 0, lists_a, 0, lists_b, 0, mid, 1)
    best_ref[...] = jnp.transpose(lists_b[pl.ds(0, TOPK, stride=SUB), :])
    heard(notes_y, ny_sem)
    flag_ref[0, 0] = jnp.max(jnp.maximum(note[1], jnp.max(notes_y[...], axis=0))).astype(jnp.int32)
    for sent in (notes_x, notes_y):
        pltpu.make_async_remote_copy(
            sent, sent, note_sem, nx_sem, device_id={"row": me}, device_id_type=MESH
        ).wait_send()


def slow_prepare(rows, list_dev, hot, cap, probes_ref, queries_ref, block_ref, enc_ref, table):
    qcount, nprobe = probes_ref.shape
    cold = rows * list_dev
    lane = lax.broadcasted_iota(jnp.int32, (qcount, cold), 1)
    ids = (lane % rows) * list_dev + lane // rows + hot
    probes = probes_ref[...]
    named = jnp.zeros((qcount, cold), jnp.float32)
    for j in range(nprobe):
        named = jnp.where(probes[:, j : j + 1] == ids, 1.0, named)
    below = lax.broadcasted_iota(jnp.int32, (qcount, qcount), 1) < lax.broadcasted_iota(
        jnp.int32, (qcount, qcount), 0
    )
    rank = jnp.dot(
        below.astype(jnp.float32).astype(jnp.bfloat16),
        named.astype(jnp.bfloat16),
        preferred_element_type=jnp.float32,
    )
    number = lax.broadcasted_iota(jnp.int32, (qcount, cold), 0).astype(jnp.float32) + 1.0
    for r in range(cap):
        held = jnp.where((named > 0) & (rank == float(r)), number, 0.0)
        line = jnp.sum(held, axis=0, keepdims=True)
        for l in range(list_dev):
            e = l * cap + r
            table[e : e + 1, :] = line[:, l * rows : (l + 1) * rows]
    half = list_dev * cap // 2
    block_ref[0:qcount, :] = queries_ref[...]
    block_ref[qcount : qcount + half, 0:rows] = table[0:half, :].astype(jnp.bfloat16)
    block_ref[qcount : qcount + half, rows : 2 * rows] = table[half : 2 * half, :].astype(
        jnp.bfloat16
    )
    columns = lax.broadcasted_iota(jnp.int32, (qcount, LANES), 1)
    enc = jnp.zeros((qcount, LANES), jnp.float32)
    for j in range(nprobe):
        p = probes[:, j : j + 1]
        mine = jnp.sum(jnp.where(p == ids, rank, 0.0), axis=1, keepdims=True)
        pf = p.astype(jnp.float32)
        code = jnp.where(p < hot, -1.0 - pf, (pf - hot) * cap + mine)
        enc = jnp.where(columns == j, code, enc)
    enc_ref[...] = jnp.transpose(enc)[0:nprobe, :].astype(jnp.int32)


def slow_exchange(rows, side, list_dev, cap, block_ref, lists_ref, out_ref, got, picked, x, y, mid, back,
             send_sem, own_sem, sib_sem, back_sem, ret_sem):
    me = lax.axis_index("row")
    mx, my, c = me // (2 * side), (me // 2) % side, me % 2
    chips = side * side
    depth = block_ref.shape[0]
    half = list_dev * cap // 2
    qcount = depth - half
    slots = list_dev * cap
    pairs = list_dev // 2

    def at(dx, dy, core):
        return (((mx + dx) % side) * side + (my + dy) % side) * 2 + core

    barrier = pltpu.get_barrier_semaphore()

    def greet(k, _):
        pl.semaphore_signal(barrier, 1, device_id={"row": (me + k) % rows}, device_id_type=MESH)
        return 0

    lax.fori_loop(1, rows, greet, 0)
    pl.semaphore_wait(barrier, rows - 1)

    def along(da, db):
        return at(da * (1 - c) + db * c, da * c + db * (1 - c), c)

    def push(src, da, db, to_a, to_b):
        slot = ((da - to_a) % side) * side + (db - to_b) % side
        pltpu.make_async_remote_copy(
            src, got.at[c, slot], send_sem, own_sem.at[slot],
            device_id={"row": along(to_a % side, to_b % side)}, device_id_type=MESH,
        ).start()

    def signed(d):
        return d if d <= side // 2 else d - side

    def forward(src, da, db):
        sa, sb = signed(da), signed(db)
        far = side // 2
        if db == 0:
            if sa <= 0 and -sa + 1 <= far and da != far:
                push(src, da, db, 1, 0)
            if sa >= 0 and sa + 1 <= far - 1:
                push(src, da, db, -1, 0)
        plus, minus = (far, far - 1) if da % 2 == 0 else (far - 1, far)
        came_plus = db == 0 or sb < 0
        came_minus = db == 0 or (sb > 0 and db != far)
        if came_plus and (0 if db == 0 else -sb) + 1 <= plus:
            push(src, da, db, 0, 1)
        if came_minus and (0 if db == 0 else sb) + 1 <= minus:
            push(src, da, db, 0, -1)

    def to_sibling(src, slot):
        pltpu.make_async_remote_copy(
            src, got.at[c, slot], send_sem, sib_sem.at[slot],
            device_id={"row": at(0, 0, 1 - c)}, device_id_type=MESH,
        ).start()

    forward(block_ref, 0, 0)
    to_sibling(block_ref, 0)
    got[c, 0] = block_ref[...]
    order = [(a, b) for a in range(side) for b in range(side) if (a, b) != (0, 0)]
    order.sort(key=lambda o: (abs(signed(o[0])) + abs(signed(o[1])), abs(signed(o[1])), o))
    for da, db in order:
        slot = da * side + db
        here = got.at[c, slot]
        pltpu.make_async_remote_copy(
            here, here, send_sem, own_sem.at[slot], device_id={"row": me}, device_id_type=MESH
        ).wait_recv()
        forward(here, da, db)
        to_sibling(here, slot)

    share = chips // (LANES // SUB)
    per = chips // share
    choose = (lax.broadcasted_iota(jnp.int32, (rows, LANES), 0) == me).astype(jnp.float32).astype(jnp.bfloat16)
    number = lax.broadcasted_iota(jnp.int32, (slots, qcount), 1).astype(jnp.float32) + 1.0
    odd = (lax.broadcasted_iota(jnp.int32, (lists_ref.shape[1], 2 * LANES), 1) // cap) % 2 == 1

    def batch(b, _):
        def take(k, _):
            i = b * per + k
            for t in range(2):
                slot = i if t == 0 else (i % side) * side + i // side
                here = got.at[t, slot]

                @pl.when((c != t))
                def _():
                    pltpu.make_async_remote_copy(
                        here, here, send_sem, sib_sem.at[slot], device_id={"row": me}, device_id_type=MESH
                    ).wait_recv()

                table = jnp.concatenate(
                    [got[t, slot, qcount:depth, 0:rows], got[t, slot, qcount:depth, rows : 2 * rows]], axis=0
                )
                wide = jnp.dot(table, choose, preferred_element_type=jnp.float32)
                hits = (wide == number).astype(jnp.float32).astype(jnp.bfloat16)
                chosen = jnp.dot(hits, got[t, slot, 0:qcount, :], preferred_element_type=jnp.float32)
                for m in range(pairs):
                    picked[m, pl.ds(pl.multiple_of(t * LANES + k * SUB, SUB), SUB), :] = chosen[
                        m * SUB : (m + 1) * SUB, :
                    ]
            return 0

        lax.fori_loop(0, per, take, 0)

        for m in range(pairs):
            right = picked[m].astype(jnp.bfloat16)
            dims = (((1,), (1,)), ((), ()))
            even_s = lax.dot_general(lists_ref[2 * m], right, dims, preferred_element_type=jnp.float32)
            odd_s = lax.dot_general(lists_ref[2 * m + 1], right, dims, preferred_element_type=jnp.float32)
            s = jnp.where(odd, odd_s, even_s)
            for t in range(2):
                x[pl.ds(2 * m + t, s.shape[0], stride=SUB), :] = s[:, t * LANES : (t + 1) * LANES]
        run(sort_top_128(x, y, mid))
        for m in range(pairs):
            for t in range(2):
                sorted_rows = jnp.transpose(y[pl.ds(2 * m + t, TOPK, stride=SUB), :])
                back[pl.ds(b * per, per), t, m * SUB : (m + 1) * SUB, :] = sorted_rows.reshape(per, SUB, TOPK)

        def give(k, _):
            i = b * per + k
            for t in range(2):

                @pl.when((i != 0) | (c != t))
                def _():
                    pltpu.make_async_remote_copy(
                        back.at[i, t], out_ref.at[me], back_sem, ret_sem,
                        device_id={"row": at(i // side, i % side, t)}, device_id_type=MESH,
                    ).start()
            return 0

        lax.fori_loop(0, per, give, 0)
        return 0

    lax.fori_loop(0, share, batch, 0)
    out_ref[me] = back[0, c]

    def drain(k, _):
        here = got.at[c, 0]
        pltpu.make_async_remote_copy(
            here, here, send_sem, own_sem.at[0], device_id={"row": me}, device_id_type=MESH
        ).wait_send()
        return 0

    lax.fori_loop(0, 2 * chips - 1, drain, 0)
    whole = out_ref.at[pl.ds(0, rows - 1)]
    done = pltpu.make_async_remote_copy(
        whole, whole, back_sem, ret_sem, device_id={"row": me}, device_id_type=MESH
    )
    done.wait_send()
    done.wait_recv()


def slow_finish(enc_smem, enc_ref, rows_ref, queries_ref, hot_ref, out_ref, buf, x, y, mid, lists_a, lists_b):
    nprobe, qcount = enc_ref.shape
    hot = hot_ref.shape[0]
    enc = enc_ref[...]

    def gather(j, _):
        def one(q, _):
            at = jnp.maximum(enc_smem[j, q], 0)
            buf[pl.ds(j * qcount + q, 1), :] = rows_ref[pl.ds(at, 1), :]
            return 0

        lax.fori_loop(0, qcount, one, 0, unroll=16)
        return 0

    lax.fori_loop(0, nprobe, gather, 0)
    for j in range(nprobe):
        dst = lists_a if j < SUB else lists_b
        flat = jnp.transpose(buf[j * qcount : (j + 1) * qcount, :])
        flat = jnp.where(enc[j : j + 1, :] < 0, NEG, flat)
        dst[pl.ds(j % SUB, TOPK, stride=SUB), :] = flat
    merge_top_128(lists_a, 0, lists_b, 0, lists_a, 0, mid)
    for g in range(hot // SUB):
        for s in range(SUB):
            h = g * SUB + s
            scores = lax.dot_general(
                hot_ref[h], queries_ref[...], (((1,), (1,)), ((), ())), preferred_element_type=jnp.float32
            )
            asked = jnp.max((enc == -1 - h).astype(jnp.float32), axis=0, keepdims=True)
            x[pl.ds(s, scores.shape[0], stride=SUB), :] = jnp.where(asked > 0, scores, NEG)
        run(sort_top_128(x, y, mid))
        merge_top_128(lists_a, 0, y, 0, lists_a, 0, mid)
    for shift in (4, 2, 1):
        merge_top_128(lists_a, 0, lists_a, 0, lists_b, 0, mid, shift)
        lists_a, lists_b = lists_b, lists_a
    out_ref[...] = jnp.transpose(lists_a[pl.ds(0, TOPK, stride=SUB), :])


def shards(queries, probes, hot_lists, cold_lists):
    rows = lax.axis_size("row")
    side = math.isqrt(rows // 2)
    qcount, nprobe = probes.shape
    width = queries.shape[1]
    list_dev, lsize = cold_lists.shape[0], cold_lists.shape[1]
    hot = hot_lists.shape[0]
    cap = 2 * ((qcount * nprobe + list_dev * rows - 1) // (list_dev * rows))
    slots = list_dev * cap
    depth = qcount + slots // 2
    vmem = pl.BlockSpec(memory_space=pltpu.VMEM)
    limit = 60 * 2**20
    f32 = jnp.float32
    column = pltpu.VMEM((lsize * SUB, LANES), f32)
    small = pltpu.VMEM((TOPK * SUB, LANES), f32)

    best, flag = pl.pallas_call(
        functools.partial(exchange, rows, side, cap),
        out_shape=(
            jax.ShapeDtypeStruct((qcount, TOPK), f32),
            jax.ShapeDtypeStruct((1, 1), jnp.int32),
        ),
        in_specs=[vmem] * 4,
        out_specs=(vmem, pl.BlockSpec(memory_space=pltpu.SMEM)),
        scratch_shapes=[
            pltpu.VMEM((depth, width), jnp.bfloat16),
            pltpu.VMEM((slots, rows), f32),
            pltpu.VMEM((qcount, rows * list_dev), f32),
            pltpu.VMEM((2, side * side, depth, width), jnp.bfloat16),
            pltpu.VMEM((list_dev // 2, 2 * LANES, width), f32),
            column,
            column,
            small,
            pltpu.VMEM((side * side, 2, slots // 2, LANES), f32),
            pltpu.VMEM((rows * slots // 2, LANES), f32),
            pltpu.VMEM((nprobe, qcount), jnp.int32),
            pltpu.VMEM((nprobe, qcount), jnp.int32),
            pltpu.SMEM((nprobe, qcount), jnp.int32),
            small,
            pltpu.VMEM((nprobe * qcount, LANES), f32),
            small,
            small,
            pltpu.VMEM((2, SUB, LANES), f32),
            pltpu.VMEM((2 * side - 1, SUB, LANES), f32),
            pltpu.VMEM((side - 1, SUB, LANES), f32),
            pltpu.SemaphoreType.DMA,
            pltpu.SemaphoreType.DMA((side * side,)),
            pltpu.SemaphoreType.DMA((side * side,)),
            pltpu.SemaphoreType.DMA,
            pltpu.SemaphoreType.DMA,
            pltpu.SemaphoreType.DMA,
            pltpu.SemaphoreType.DMA,
            pltpu.SemaphoreType.DMA,
            pltpu.SemaphoreType.DMA,
        ],
        compiler_params=pltpu.CompilerParams(collective_id=0, has_side_effects=True, vmem_limit_bytes=limit),
    )(probes.T, queries, cold_lists, hot_lists)

    def full(best, queries, probes, hot_lists, cold_lists):
        block, enc = pl.pallas_call(
            functools.partial(slow_prepare, rows, list_dev, hot, cap),
            out_shape=(
                jax.ShapeDtypeStruct((depth, width), jnp.bfloat16),
                jax.ShapeDtypeStruct((nprobe, qcount), jnp.int32),
            ),
            in_specs=[vmem] * 2,
            out_specs=(vmem, vmem),
            scratch_shapes=[pltpu.VMEM((slots, rows), f32)],
            compiler_params=pltpu.CompilerParams(vmem_limit_bytes=limit),
        )(probes, queries)
        returned = pl.pallas_call(
            functools.partial(slow_exchange, rows, side, list_dev, cap),
            out_shape=jax.ShapeDtypeStruct((rows, slots, TOPK), f32),
            in_specs=[vmem] * 2,
            out_specs=vmem,
            scratch_shapes=[
                pltpu.VMEM((2, side * side, depth, width), jnp.bfloat16),
                pltpu.VMEM((list_dev // 2, 2 * LANES, width), f32),
                column,
                column,
                small,
                pltpu.VMEM((side * side, 2, slots, TOPK), f32),
                pltpu.SemaphoreType.DMA,
                pltpu.SemaphoreType.DMA((side * side,)),
                pltpu.SemaphoreType.DMA((side * side,)),
                pltpu.SemaphoreType.DMA,
                pltpu.SemaphoreType.DMA,
            ],
            compiler_params=pltpu.CompilerParams(collective_id=1, has_side_effects=True, vmem_limit_bytes=limit),
        )(block, cold_lists)
        return pl.pallas_call(
            slow_finish,
            out_shape=jax.ShapeDtypeStruct((qcount, TOPK), f32),
            in_specs=[pl.BlockSpec(memory_space=pltpu.SMEM)] + [vmem] * 4,
            out_specs=vmem,
            scratch_shapes=[pltpu.VMEM((nprobe * qcount, TOPK), f32), column, column, small, small, small],
            compiler_params=pltpu.CompilerParams(vmem_limit_bytes=limit),
        )(enc, enc, returned.reshape(rows * slots, TOPK), queries, hot_lists)

    return lax.cond(
        flag[0, 0] > 0, full, lambda best, *_: best, best, queries, probes, hot_lists, cold_lists
    )


def solution(mesh):
    placed = (
        P(("tenant", "row"), None),
        P(("tenant", "row"), None),
        P("tenant", None, None),
        P(("tenant", "row"), None, None),
    )
    return jax.shard_map(
        shards, mesh=mesh, in_specs=placed, out_specs=P(("tenant", "row"), None), check_vma=False
    )
```
